128 devices in a mesh: row: 8 (over y_hi, z), col: 16 (over x, y_lo, core).
Axes of the slice: x: 4, y: 4 (y_hi: 2, y_lo: 2; y = y_hi * 2 + y_lo), z: 4, core: 2. Of those that a mesh axis runs over, the one named last changes fastest.
Arguments:
- region: float32 [8, 1024, 8, 1024], P(None, 'col', None, 'row'), may hold values from -6 to 6
- l_panels: bfloat16 [3, 1024, 11, 1024], P(None, 'col', None, 'row'), may hold values from -0.0625 to 0.0625
- u_panels: bfloat16 [3, 11, 1024, 1024], P(None, None, 'col', 'row'), may hold values from -0.0625 to 0.0625
- diag_inv: float32 [3, 1024, 1024], P(None, 'col', 'row'), may hold values from -6 to 6
- pattern: int32 [3, 11, 8], replicated, may hold values from 0 to 1, as said below
Outputs:
- inverse: float32 [11, 1024, 11, 1024], P(None, 'col', None, 'row')
The draws below stay inside these ranges and needn't reach their ends.
Inputs may be any that keep to these rules, and one draw needn't show every extreme that they name: pattern[s] marks the 128-row blocks in the structure of supernode s: only blocks of segments after s; for the last supernode only blocks of the ancestor region; for every other supernode all blocks of one later supernode (its parent in the elimination tree) and otherwise only blocks that the parent's pattern also marks.
All inputs are finite; a program needn't handle non-finite values.
Results may differ from the reference program's by a relative error of at most 0.0003.
Values may be sent and summed in bfloat16 or wider, within the bound.
A program may use at most 128 MiB of HBM per device.

```python
import jax
import jax.numpy as jnp
from jax import lax

W = 1024
BLK = 128
NSUP = 3
ASEG = 8
NSEG = 11
WB = 8


def draw_pattern(key, part):
    seg_index = jnp.arange(NSEG, dtype=jnp.int32)[:, None] * jnp.ones((1, WB), jnp.int32)
    structs = jnp.zeros((NSUP, NSEG, WB), jnp.int32)
    region_bits = jax.random.randint(jax.random.fold_in(key, 7), (NSEG, WB), 0, 2)
    structs = structs.at[NSUP - 1].set(region_bits * (seg_index >= NSUP).astype(jnp.int32))
    for level in range(NSUP - 2, -1, -1):
        parent = jax.random.randint(jax.random.fold_in(key, 100 + level), (), level + 1, NSUP)
        kept_bits = (jax.random.randint(jax.random.fold_in(key, 200 + level), (NSEG, WB), 0, 4) > 0).astype(jnp.int32)
        parent_blocks = (seg_index == parent).astype(jnp.int32)
        structs = structs.at[level].set(jnp.maximum(parent_blocks, structs[parent] * kept_bits))
    return structs


def steps_of(stream_key, shape, cuts, smallest, top_value):
    def one(position, parts):
        heights = jax.random.uniform(jax.random.fold_in(jax.random.fold_in(stream_key, 6), position), (parts,), jnp.float32, smallest / len(cuts), top_value / len(cuts))
        return jnp.repeat(jnp.exp(heights), shape[position] // parts).reshape((-1,) + (1,) * (len(shape) - position - 1))

    gain = one(*cuts[0])
    for cut in cuts[1:]:
        gain = gain * one(*cut)
    return gain


def bell_draw(stream_key, shape, width, bound, shards=(), kind=jnp.bfloat16):
    loudness = steps_of(stream_key, shape, shards, -0.22, 0.18) if shards else 1.0
    entries = jax.random.normal(stream_key, shape, jnp.float32) * width * loudness
    return jnp.minimum(jnp.maximum(entries, -bound), bound).astype(kind)


def setup_inputs(seed: int = 0) -> dict:
    streams_of = jax.random.split(jax.random.key(seed), 6)
    return {
        "region": bell_draw(streams_of[0], (ASEG, W, ASEG, W), 1.0, 6.0, ((1, 16), (3, 8)), jnp.float32),
        "l_panels": bell_draw(streams_of[1], (NSUP, W, NSEG, W), (ASEG * W) ** -0.5, 0.0625, ((1, 16), (3, 8))),
        "u_panels": bell_draw(streams_of[2], (NSUP, NSEG, W, W), (ASEG * W) ** -0.5, 0.0625, ((2, 16), (3, 8))),
        "diag_inv": bell_draw(streams_of[3], (NSUP, W, W), 1.0, 6.0, ((1, 16), (2, 8)), jnp.float32),
        "pattern": draw_pattern(jax.random.fold_in(streams_of[5], 71), 0),
    }


def reference(region, l_panels, u_panels, diag_inv, pattern):
    inverse = jnp.zeros((NSEG, W, NSEG, W), jnp.float32)
    inverse = inverse.at[NSUP:, :, NSUP:, :].set(region.astype(jnp.float32))
    block_mask = jnp.repeat(pattern.astype(jnp.float32), BLK, axis=2)
    for level in reversed(range(NSUP)):
        mask_now = block_mask[level]
        lower = l_panels[level].astype(jnp.float32) * mask_now[None, :, :]
        upper = u_panels[level].astype(jnp.float32) * mask_now[:, :, None]
        column = -mask_now[:, :, None] * jnp.einsum("ajbk,wbk->ajw", inverse, lower, precision=lax.Precision.HIGHEST)
        row_panel = -mask_now[None, :, :] * jnp.einsum("akw,akbj->wbj", upper, inverse, precision=lax.Precision.HIGHEST)
        diagonal = diag_inv[level] - jnp.einsum("akw,akv->wv", upper, column, precision=lax.Precision.HIGHEST)
        inverse = inverse.at[:, :, level, :].set(column)
        inverse = inverse.at[level].set(row_panel)
        inverse = inverse.at[level, :, level, :].set(diagonal)
    return inverse
```

```python
import jax
import jax.numpy as jnp
from jax import lax
from jax.experimental import pallas as pl
from jax.experimental.pallas import tpu as pltpu
from jax.sharding import Mesh
from jax.sharding import PartitionSpec as P

F32 = jnp.float32
BF16 = jnp.bfloat16
BLK = 128
NSUP = 3
NSEG = 11
ROW = ("yh", "z")
COL = ("x", "yl", "core")
ORDER = (3, 4, 5, 6, 7, 8, 9, 10, 2, 1)
NK = {2: 8, 1: 9, 0: 10}
KC = {2: 1024, 1: 1152, 0: 1280}
KR = {2: 512, 1: 576, 0: 640}
UL = {2: 512, 1: 640, 0: 640}
BUF = {2: 0, 1: 1, 0: 0}
MESH = pl.DeviceIdType.MESH


def nt(a, b):
    return lax.dot_general(a, b, (((1,), (1,)), ((), ())), preferred_element_type=F32)


def nn(a, b):
    return lax.dot_general(a, b, (((1,), (0,)), ((), ())), preferred_element_type=F32)


def split(v):
    hi = v.astype(BF16)
    return hi, (v - hi.astype(F32)).astype(BF16)


class Sems:
    def __init__(self, ref):
        self.ref, self.used = ref, 0

    def take(self):
        self.used += 1
        return self.ref.at[self.used - 1]


def kernel(mr, mc, reg, lin, uin, diag, out, a32, kh, kl, ls2, ls1, ls0, us2, us1, us0, cp, rp, rcl,
           rrl, rxl, ryl, crl, cxl, cyl, dp, dl, cf, rf, df, rh, rl, send_sem, recv_sem, out_sem):
    ls = {2: ls2, 1: ls1, 0: ls0}
    us = {2: us2, 1: us1, 0: us0}
    yh, z = lax.axis_index("yh"), lax.axis_index("z")
    x, yl, core = lax.axis_index("x"), lax.axis_index("yl"), lax.axis_index("core")
    sends, recvs, outs = Sems(send_sem), Sems(recv_sem), Sems(out_sem)
    out_copies = []

    def remote(src, dst, where):
        return pltpu.make_async_remote_copy(
            src_ref=src, dst_ref=dst, send_sem=sends.take(), recv_sem=recvs.take(),
            device_id=where, device_id_type=MESH)

    def to_out(src, dst):
        copy = pltpu.make_async_copy(src, dst, outs.take())
        copy.start()
        out_copies.append(copy)

    def ring_places(axis, here):
        return {axis: lax.rem(here + 1, 4)}, {axis: lax.rem(here + 3, 4)}

    loads = [pltpu.make_async_copy(reg.at[:, :, b, :], a32.at[b], outs.take()) for b in range(8)]
    for copy in loads:
        copy.start()
    barrier = pltpu.get_barrier_semaphore()
    peers = [{"yl": 1 - yl}, {"core": 1 - core}, *ring_places("x", x)]
    others = [(a, d) for a in range(2) for d in range(4) if (a, d) != (0, 0)]
    peers += [{"yh": lax.rem(yh + a, 2), "z": lax.rem(z + d, 4)} for a, d in others]
    for peer in peers:
        pl.semaphore_signal(barrier, inc=1, device_id=peer, device_id_type=MESH)
    pl.semaphore_wait(barrier, len(peers))

    def gather(src, slab, axis, here, pair_axis, pair, to_core):
        up, down = ring_places(axis, here)
        hp, hm, h2 = lax.rem(here + 1, 4), lax.rem(here + 3, 4), lax.rem(here + 2, 4)
        other = {pair_axis: 1 - pair}
        oq = 1 - pair
        started, crossed = [], []

        def go(copy):
            copy.start()
            started.append(copy)
            return copy

        def cross(h, q):
            if to_core:
                crossed.append(go(remote(slab(h, q), slab(h, q), {"core": 1 - core})))

        slab(here, pair)[...] = src[...]
        m_pair = go(remote(src, slab(here, pair), other))
        m_op = go(remote(src, slab(here, pair), up))
        m_om = go(remote(src, slab(here, pair), down))
        if to_core:
            crossed.append(go(remote(src, slab(here, pair), {"core": 1 - core})))
        yield
        m_pair.wait_recv()
        m_tp = go(remote(slab(here, oq), slab(here, oq), up))
        m_tm = go(remote(slab(here, oq), slab(here, oq), down))
        cross(here, oq)
        m_op.wait_recv()
        m_rp = go(remote(slab(hm, pair), slab(hm, pair), up))
        cross(hm, pair)
        m_om.wait_recv()
        cross(hp, pair)
        yield
        m_tm.wait_recv()
        m_rm = go(remote(slab(hp, oq), slab(hp, oq), down))
        cross(hp, oq)
        m_tp.wait_recv()
        cross(hm, oq)
        yield
        m_rp.wait_recv()
        cross(h2, pair)
        m_rm.wait_recv()
        cross(h2, oq)
        yield
        for copy in crossed:
            copy.wait_recv()
        for copy in started:
            copy.wait_send()
        yield

    def gather_l(s):
        slab = ls[s]
        return gather(lin.at[s, :, 0:KC[s]], lambda h, q: slab.at[(h * 2 + q) * 2 + core], "x", x, "yl", yl, True)

    def gather_u(s):
        slab = us[s]
        return gather(uin.at[s, :, 0:UL[s]], lambda h, q: slab.at[q * 4 + h], "z", z, "yh", yh, False)

    def reduce_ring(blk, relay, side, last, axis, here, pair_axis, pair, pre, finish):
        up, down = ring_places(axis, here)
        hp, hm, h2 = lax.rem(here + 1, 4), lax.rem(here + 3, 4), lax.rem(here + 2, 4)
        started = []

        def go(src, dst, where):
            copy = remote(src, dst, where)
            copy.start()
            started.append(copy)
            return copy

        pre(h2, 0)
        m_rp = go(blk(h2, 0), relay(0), up)
        pre(h2, 1)
        m_rm = go(blk(h2, 1), relay(1), down)
        pre(hp, 1)
        m_ep = go(blk(hp, 1), side(0, 1), up)
        pre(hm, 0)
        m_em = go(blk(hm, 0), side(1, 0), down)
        pre(hp, 0)
        pre(hm, 1)
        pre(here, 0)
        pre(here, 1)
        yield
        m_rp.wait_recv()
        blk(hp, 0)[...] += relay(0)[...]
        m_fp = go(blk(hp, 0), side(0, 0), up)
        m_rm.wait_recv()
        blk(hm, 1)[...] += relay(1)[...]
        m_fm = go(blk(hm, 1), side(1, 1), down)
        yield
        for copy in (m_ep, m_em, m_fp, m_fm):
            copy.wait_recv()
        oq = 1 - pair
        blk(here, oq)[...] += side(0, oq)[...] + side(1, oq)[...]
        m_y = go(blk(here, oq), last, {pair_axis: oq})
        blk(here, pair)[...] += side(0, pair)[...] + side(1, pair)[...]
        yield
        m_y.wait_recv()
        finish()
        for copy in started:
            copy.wait_send()
        yield

    def reduce_rows(s):
        b, n = BUF[s], KC[s]
        blk = lambda h, q: rp.at[b, core, h * 2 + q, :, 0:n]
        over = remote(rp.at[b, 1 - core, :, :, 0:n], rcl.at[b, :, :, 0:n], {"core": 1 - core})
        over.start()
        yield
        over.wait_recv()

        def pre(h, q):
            blk(h, q)[...] += rcl[b, h * 2 + q, :, 0:n]

        def finish():
            for i in range(NK[s]):
                at = slice(i * 128, (i + 1) * 128)
                v = mc[s, i] * (rp[b, core, x * 2 + yl, :, at] + ryl[b, :, at])
                rf[s, :, at] = v
                hi, lo = split(v)
                rh[:, at] = hi
                rl[:, at] = lo
                if s > 0:
                    r0 = 512 + 64 * (2 - s)
                    kh[r0 : r0 + 64, at] = hi
                    kl[r0 : r0 + 64, at] = lo
                to_out(rf.at[s, :, at], out.at[s, :, ORDER[i], :])

        yield from reduce_ring(
            blk, lambda d: rrl.at[b, d, :, 0:n], lambda d, q: rxl.at[b, d, q, :, 0:n], ryl.at[b, :, 0:n],
            "x", x, "yl", yl, pre, finish)
        over.wait_send()
        yield

    def reduce_cols(s):
        b, n = BUF[s], KR[s]
        blk = lambda h, q: cp.at[b, q * 4 + h, 0:n, :]

        def finish():
            for i in range(NK[s]):
                at = slice(i * 64, (i + 1) * 64)
                v = mr[s, i] * (cp[b, yh * 4 + z, at, :] + cyl[b, at, :])
                cf[s, i] = v
                if s > 0:
                    c0 = 1024 + 128 * (2 - s)
                    hi, lo = split(v)
                    kh[at, c0 : c0 + 128] = hi
                    kl[at, c0 : c0 + 128] = lo
            to_out(cf.at[s, 0:8], out.at[3:11, :, s, :])
            for i in range(8, NK[s]):
                to_out(cf.at[s, i], out.at[ORDER[i], :, s, :])

        yield from reduce_ring(
            blk, lambda d: crl.at[b, d, 0:n, :], lambda d, q: cxl.at[b, d, q, 0:n, :], cyl.at[b, 0:n, :],
            "z", z, "yh", yh, lambda h, q: None, finish)

    def reduce_diag(s):
        b, n = BUF[s], KC[s]

        @pl.loop(0, 4)
        def _(t):
            w = ls[s][pl.ds(4 * t, 4), :, :].reshape(256, n)
            acc = nt(rh[:, 0:n], w) + nt(rl[:, 0:n], w)
            dp[b, 2 * t] = acc[:, 0:128]
            dp[b, 2 * t + 1] = acc[:, 128:256]

        started = []
        for k, (a, d) in enumerate(others):
            py, pz = lax.rem(yh + a, 2), lax.rem(z + d, 4)
            copy = remote(dp.at[b, py * 4 + pz], dl.at[b, k], {"yh": py, "z": pz})
            copy.start()
            started.append(copy)
        yield
        for copy in started:
            copy.wait_recv()
        v = diag[s] - dp[b, yh * 4 + z]
        for k in range(7):
            v = v - dl[b, k]
        df[s] = v
        if s > 0:
            r0, c0 = 512 + 64 * (2 - s), 1024 + 128 * (2 - s)
            hi, lo = split(v)
            kh[r0 : r0 + 64, c0 : c0 + 128] = hi
            kl[r0 : r0 + 64, c0 : c0 + 128] = lo
        to_out(df.at[s], out.at[s, :, s, :])
        for copy in started:
            copy.wait_send()
        yield

    def store_r(b, t, acc, at):
        for q in range(4):
            rp[b, q % 2, 2 * t + q // 2, :, at] = acc[64 * q : 64 * (q + 1), :]

    def heavy_c(s):
        b = BUF[s]

        @pl.loop(0, 4)
        def _(t):
            w = ls[s][pl.ds(4 * t, 4), :, 0:1024].reshape(256, 1024)
            acc = nt(kh[0:512, 0:1024], w) + nt(kl[0:512, 0:1024], w)
            cp[b, 2 * t, 0:512, :] = acc[:, 0:128]
            cp[b, 2 * t + 1, 0:512, :] = acc[:, 128:256]

    def heavy_r(s):
        b = BUF[s]

        @pl.loop(0, 4)
        def _(t):
            w = us[s][pl.ds(2 * t, 2), :, 0:512].reshape(256, 512)
            acc = nn(w, kh[0:512, 0:1024]) + nn(w, kl[0:512, 0:1024])
            store_r(b, t, acc, slice(0, 1024))

    def extra(s):
        b, n, m = BUF[s], KC[s], KR[s]

        @pl.loop(0, 4)
        def _(t):
            w = us[s][pl.ds(2 * t, 2), :, :].reshape(256, 640)
            acc = nn(w[:, 512:640], kh[512:640, 0:1024]) + nn(w[:, 512:640], kl[512:640, 0:1024])
            for q in range(4):
                rp[b, q % 2, 2 * t + q // 2, :, 0:1024] += acc[64 * q : 64 * (q + 1), :]
            acc = nn(w, kh[0:640, 1024:n]) + nn(w, kl[0:640, 1024:n])
            store_r(b, t, acc, slice(1024, n))

        @pl.loop(0, 4)
        def _(t):
            w = ls[s][pl.ds(4 * t, 4), :, :].reshape(256, n)
            acc = nt(kh[0:512, 1024:n], w[:, 1024:n]) + nt(kl[0:512, 1024:n], w[:, 1024:n])
            cp[b, 2 * t, 0:512, :] += acc[:, 0:128]
            cp[b, 2 * t + 1, 0:512, :] += acc[:, 128:256]
            acc = nt(kh[512:m, 0:n], w) + nt(kl[512:m, 0:n], w)
            cp[b, 2 * t, 512:m, :] = acc[:, 0:128]
            cp[b, 2 * t + 1, 512:m, :] = acc[:, 128:256]

    gl = {s: gather_l(s) for s in (2, 1, 0)}
    gu = {s: gather_u(s) for s in (2, 1, 0)}

    def step_gather(s):
        next(gl[s])
        next(gu[s])

    step_gather(2)
    for b in range(8):
        loads[b].wait()
        to_out(a32.at[b], out.at[3:11, :, 3 + b, :])
        hi, lo = split(a32[b].reshape(512, 128))
        kh[0:512, b * 128 : (b + 1) * 128] = hi
        kl[0:512, b * 128 : (b + 1) * 128] = lo
    for ref in (kh, kl):
        ref[512:640, :] = jnp.zeros((128, 1280), BF16)
        ref[0:512, 1024:1280] = jnp.zeros((512, 256), BF16)
    for _ in range(4):
        step_gather(2)
    step_gather(1)
    heavy_r(2)
    heavy_c(2)
    for s in (2, 1, 0):
        t = s - 1
        if t >= 0:
            after = [lambda: step_gather(t)] * 4 + [lambda: heavy_r(t), lambda: heavy_c(t)]
            if t == 1:
                after.append(lambda: step_gather(0))
        else:
            after = []

        def fill(count):
            for _ in range(count):
                if after:
                    after.pop(0)()

        r, c = reduce_rows(s), reduce_cols(s)
        next(r)
        next(c)
        fill(1)
        next(r)
        next(c)
        fill(1)
        next(r)
        next(c)
        fill(2)
        next(r)
        next(c)
        fill(1)
        next(r)
        d = reduce_diag(s)
        next(d)
        next(r)
        fill(9)
        next(d)
        if t >= 0:
            extra(t)
    for copy in out_copies:
        copy.wait()


def per_device(region, l_panels, u_panels, diag_inv, pattern):
    row_index = lax.axis_index(ROW)
    col_index = lax.axis_index(COL)
    order = jnp.array(ORDER)
    picked = pattern[:, order, :]
    rows_block = col_index // 2
    mr = lax.dynamic_slice_in_dim(picked, rows_block, 1, 2)[:, :, 0]
    mc = lax.dynamic_slice_in_dim(picked, row_index, 1, 2)[:, :, 0]

    def in_order(value, dim):
        cut = lambda a, b: lax.slice_in_dim(value, a, b, axis=dim)
        return jnp.concatenate([cut(3, 11), cut(2, 3), cut(1, 2)], axis=dim)

    lin = in_order(l_panels, 2) * mc.astype(BF16)[:, None, :, None]
    lin = lin.reshape(3, 64, 1280)
    uin = in_order(u_panels, 1) * mr.astype(BF16)[:, :, None, None]
    uin = uin.transpose(0, 3, 1, 2).reshape(3, 128, 640)
    smem = pl.BlockSpec(memory_space=pltpu.SMEM)
    vmem = pl.BlockSpec(memory_space=pltpu.VMEM)
    hbm = pl.BlockSpec(memory_space=pl.ANY)
    sem = lambda n: pltpu.SemaphoreType.DMA((n,))
    return pl.pallas_call(
        kernel,
        name="selinv",
        out_shape=jax.ShapeDtypeStruct((NSEG, 64, NSEG, 128), F32),
        in_specs=[smem, smem, hbm, vmem, vmem, vmem],
        out_specs=hbm,
        scratch_shapes=[
            pltpu.VMEM((8, 8, 64, 128), F32),
            pltpu.VMEM((640, 1280), BF16),
            pltpu.VMEM((640, 1280), BF16),
            pltpu.VMEM((16, 64, KC[2]), BF16),
            pltpu.VMEM((16, 64, KC[1]), BF16),
            pltpu.VMEM((16, 64, KC[0]), BF16),
            pltpu.VMEM((8, 128, UL[2]), BF16),
            pltpu.VMEM((8, 128, UL[1]), BF16),
            pltpu.VMEM((8, 128, UL[0]), BF16),
            pltpu.VMEM((2, 8, 640, 128), F32),
            pltpu.VMEM((2, 2, 8, 64, 1280), F32),
            pltpu.VMEM((2, 8, 64, 1280), F32),
            pltpu.VMEM((2, 2, 64, 1280), F32),
            pltpu.VMEM((2, 2, 2, 64, 1280), F32),
            pltpu.VMEM((2, 64, 1280), F32),
            pltpu.VMEM((2, 2, 640, 128), F32),
            pltpu.VMEM((2, 2, 2, 640, 128), F32),
            pltpu.VMEM((2, 640, 128), F32),
            pltpu.VMEM((2, 8, 64, 128), F32),
            pltpu.VMEM((2, 7, 64, 128), F32),
            pltpu.VMEM((3, 10, 64, 128), F32),
            pltpu.VMEM((3, 64, 1280), F32),
            pltpu.VMEM((3, 64, 128), F32),
            pltpu.VMEM((64, 1280), BF16),
            pltpu.VMEM((64, 1280), BF16),
            sem(160),
            sem(160),
            sem(64),
        ],
        compiler_params=pltpu.CompilerParams(
            collective_id=0, has_side_effects=True, vmem_limit_bytes=64000 * 1024),
    )(-mr.astype(F32), -mc.astype(F32), region, lin, uin, diag_inv)


def solution(mesh):
    split_mesh = Mesh(mesh.devices.reshape(2, 4, 4, 2, 2), ROW + COL)
    in_specs = (
        P(None, COL, None, ROW),
        P(None, COL, None, ROW),
        P(None, None, COL, ROW),
        P(None, COL, ROW),
        P(),
    )
    out_specs = P(None, COL, None, ROW)
    return jax.shard_map(
        per_device, mesh=split_mesh, in_specs=in_specs, out_specs=out_specs, check_vma=False
    )
```

```python
import jax
import jax.numpy as jnp
from jax import lax
from jax.experimental import pallas as pl
from jax.experimental.pallas import tpu as pltpu
from jax.sharding import Mesh
from jax.sharding import PartitionSpec as P

F32 = jnp.float32
BF16 = jnp.bfloat16
I16 = jnp.int16
NSEG = 11
ROW = ("yh", "z")
COL = ("x", "yl", "core")
KC = {2: 1024, 1: 1152, 0: 1280}
KR = {2: 512, 1: 576, 0: 640}
U0 = {2: 128, 1: 0, 0: 0}
BUF = {2: 0, 1: 1, 0: 0}
TOP = 32700.0
MESH = pl.DeviceIdType.MESH


def nt(a, b):
    return lax.dot_general(a, b, (((1,), (1,)), ((), ())), preferred_element_type=F32)


def nn(a, b):
    return lax.dot_general(a, b, (((1,), (0,)), ((), ())), preferred_element_type=F32)


def split(v):
    hi = v.astype(BF16)
    return hi, (v - hi.astype(F32)).astype(BF16)


def folded(v):
    return v.reshape(v.shape[0] // 8, 8, 128)


class Sems:
    def __init__(self, ref):
        self.ref, self.used = ref, 0

    def take(self):
        self.used += 1
        return self.ref.at[self.used - 1]


def kernel(pattern, reg, lin, uin, diag, out, a32, kh, kl, ls2, ls1, ls0, us2, us1, us0, cp, rp, rcl,
           rq_out, rq_in, rs_out, rs_in, cq_out, cq_in, cs_out, cs_in, dp, dl, cf, rf, df, rh, rl,
           send_sem, recv_sem, out_sem):
    ls = {2: ls2, 1: ls1, 0: ls0}
    us = {2: us2, 1: us1, 0: us0}
    yh, z = lax.axis_index("yh"), lax.axis_index("z")
    x, yl, core = lax.axis_index("x"), lax.axis_index("yl"), lax.axis_index("core")
    sends, recvs, outs = Sems(send_sem), Sems(recv_sem), Sems(out_sem)
    out_copies = []

    def mask_row(s, i):
        return pattern[s, i + 1, x * 2 + yl].astype(F32)

    def mask_col(s, i):
        return pattern[s, i + 1, yh * 4 + z].astype(F32)

    def remote(src, dst, where):
        return pltpu.make_async_remote_copy(
            src_ref=src, dst_ref=dst, send_sem=sends.take(), recv_sem=recvs.take(),
            device_id=where, device_id_type=MESH)

    def to_out(src, dst):
        copy = pltpu.make_async_copy(src, dst, outs.take())
        copy.start()
        out_copies.append(copy)

    def ring_places(axis, here):
        return {axis: lax.rem(here + 1, 4)}, {axis: lax.rem(here + 3, 4)}

    others = [(a, d) for a in range(2) for d in range(4) if (a, d) != (0, 0)]
    with jax.named_scope("signal"):
        barrier = pltpu.get_barrier_semaphore()
        peers = [{"yl": 1 - yl}, {"core": 1 - core}, *ring_places("x", x)]
        peers += [{"yh": lax.rem(yh + a, 2), "z": lax.rem(z + d, 4)} for a, d in others]
        for peer in peers:
            pl.semaphore_signal(barrier, inc=1, device_id=peer, device_id_type=MESH)
    loads = [pltpu.make_async_copy(reg.at[:, :, b, :], a32.at[b], outs.take()) for b in range(8)]
    for copy in loads:
        copy.start()
    with jax.named_scope("own"):
        lane = lax.broadcasted_iota(jnp.int32, (128, 128), 1)
        for s in (2, 1, 0):
            for i in range(s, 10):
                v = lin[s, :, 128 * i : 128 * (i + 1)].astype(F32) * mask_col(s, i)
                ls[s][(x * 2 + yl) * 2 + core, :, 128 * (i - s) : 128 * (i - s + 1)] = v.astype(BF16)
            for i in range(U0[s] // 128, 5):
                m = jnp.where(lane < 64, mask_row(s, 2 * i), mask_row(s, 2 * i + 1))
                v = uin[s, :, 128 * i : 128 * (i + 1)].astype(F32) * m
                us[s][yh * 4 + z, :, 128 * i - U0[s] : 128 * (i + 1) - U0[s]] = v.astype(BF16)
    with jax.named_scope("barrier"):
        pl.semaphore_wait(barrier, len(peers))

    def gather(slab, axis, here, pair_axis, pair, to_core):
        up, down = ring_places(axis, here)
        hp, hm, h2 = lax.rem(here + 1, 4), lax.rem(here + 3, 4), lax.rem(here + 2, 4)
        other = {pair_axis: 1 - pair}
        oq = 1 - pair
        started, crossed = [], []

        def go(copy):
            copy.start()
            started.append(copy)
            return copy

        def cross(h, q):
            if to_core:
                crossed.append(go(remote(slab(h, q), slab(h, q), {"core": 1 - core})))

        src = slab(here, pair)
        m_pair = go(remote(src, slab(here, pair), other))
        m_op = go(remote(src, slab(here, pair), up))
        m_om = go(remote(src, slab(here, pair), down))
        if to_core:
            crossed.append(go(remote(src, slab(here, pair), {"core": 1 - core})))
        yield
        m_pair.wait_recv()
        m_tp = go(remote(slab(here, oq), slab(here, oq), up))
        m_tm = go(remote(slab(here, oq), slab(here, oq), down))
        cross(here, oq)
        m_op.wait_recv()
        m_rp = go(remote(slab(hm, pair), slab(hm, pair), up))
        cross(hm, pair)
        m_om.wait_recv()
        cross(hp, pair)
        yield
        m_tm.wait_recv()
        m_rm = go(remote(slab(hp, oq), slab(hp, oq), down))
        cross(hp, oq)
        m_tp.wait_recv()
        cross(hm, oq)
        yield
        m_rp.wait_recv()
        cross(h2, pair)
        m_rm.wait_recv()
        cross(h2, oq)
        yield
        for copy in crossed:
            copy.wait_recv()
        for copy in started:
            copy.wait_send()
        yield

    def gather_l(s):
        slab = ls[s]
        return gather(lambda h, q: slab.at[(h * 2 + q) * 2 + core], "x", x, "yl", yl, True)

    def gather_u(s):
        slab = us[s]
        return gather(lambda h, q: slab.at[q * 4 + h], "z", z, "yh", yh, False)

    def reduce_ring(tiles, val, q_out, q_in, s_out, s_in, part, axis, here, pair_axis, pair, keep, finish):
        up, down = ring_places(axis, here)
        hp, hm, h2 = lax.rem(here + 1, 4), lax.rem(here + 3, 4), lax.rem(here + 2, 4)
        oq = 1 - pair
        started = []

        def send(k, values, where):
            top = None
            for v in values:
                m = jnp.max(folded(jnp.abs(v)), axis=0)
                top = m if top is None else jnp.maximum(top, m)
            top = jnp.maximum(top, 1e-30)
            s_out[k] = top * (1.0 / TOP)
            inv = TOP / top
            for j, v in enumerate(values):
                q = jnp.round(folded(v) * inv).reshape(v.shape)
                q_out.at[k].at[part(j)][...] = q.astype(jnp.int32).astype(I16)
            pair_of = (remote(q_out.at[k].at[part(None)], q_in.at[k].at[part(None)], where),
                       remote(s_out.at[k], s_in.at[k], where))
            for copy in pair_of:
                copy.start()
            started.extend(pair_of)
            return pair_of

        def arrive(*messages):
            for pair_of in messages:
                for copy in pair_of:
                    copy.wait_recv()

        def got(k, j):
            v = q_in.at[k].at[part(j)][...].astype(F32)
            return (folded(v) * s_in[k]).reshape(v.shape)

        each = range(tiles)
        m_rp = send(0, [val(h2, 0, j) for j in each], up)
        m_rm = send(1, [val(h2, 1, j) for j in each], down)
        m_ep = send(3, [val(hp, 1, j) for j in each], up)
        m_em = send(4, [val(hm, 0, j) for j in each], down)
        yield
        arrive(m_rp)
        m_fp = send(2, [val(hp, 0, j) + got(0, j) for j in each], up)
        arrive(m_rm)
        m_fm = send(5, [val(hm, 1, j) + got(1, j) for j in each], down)
        yield
        arrive(m_ep, m_em, m_fp, m_fm)
        m_y = send(6, [val(here, oq, j) + got(2 + oq, j) + got(4 + oq, j) for j in each], {pair_axis: oq})
        for j in each:
            keep(j, val(here, pair, j) + got(2 + pair, j) + got(4 + pair, j))
        yield
        arrive(m_y)
        for j in each:
            finish(j, got(6, j))
        for copy in started:
            copy.wait_send()
        yield

    def reduce_rows(s):
        b, c0 = BUF[s], 128 * s
        over = remote(rp.at[b, 1 - core, :, :, c0:1280], rcl.at[b, :, :, c0:1280], {"core": 1 - core})
        over.start()
        yield
        over.wait_recv()

        def cols(j):
            return slice(c0 + 128 * j, c0 + 128 * (j + 1))

        def part(j):
            return (slice(0, 64), slice(c0, 1280) if j is None else cols(j))

        def val(h, q, j):
            return rp[b, core, h * 2 + q, :, cols(j)] + rcl[b, h * 2 + q, :, cols(j)]

        def keep(j, v):
            rf[s, :, cols(j)] = v

        def finish(j, last):
            at = cols(j)
            v = -mask_col(s, s + j) * (rf[s, :, at] + last)
            rf[s, :, at] = v
            hi, lo = split(v)
            rh[:, at] = hi
            rl[:, at] = lo
            if s > 0:
                kh[64 * (s - 1) : 64 * s, at] = hi
                kl[64 * (s - 1) : 64 * s, at] = lo
            to_out(rf.at[s, :, at], out.at[s, :, s + j + 1, :])

        yield from reduce_ring(
            10 - s, val, rq_out.at[b], rq_in.at[b], rs_out.at[b], rs_in.at[b], part,
            "x", x, "yl", yl, keep, finish)
        over.wait_send()
        yield

    def reduce_cols(s):
        b, r0 = BUF[s], 64 * s
        rows = slice(r0, 640)

        def keep(j, v):
            cf[s, rows, :] = v

        def finish(j, last):
            for i in range(s, 10):
                at = slice(64 * i, 64 * (i + 1))
                v = -mask_row(s, i) * (cf[s, at, :] + last[64 * (i - s) : 64 * (i - s + 1), :])
                cf[s, at, :] = v
                if s > 0:
                    hi, lo = split(v)
                    kh[at, 128 * (s - 1) : 128 * s] = hi
                    kl[at, 128 * (s - 1) : 128 * s] = lo
                to_out(cf.at[s, at, :], out.at[i + 1, :, s, :])

        yield from reduce_ring(
            1, lambda h, q, j: cp[b, q * 4 + h, rows, :], cq_out.at[b], cq_in.at[b], cs_out.at[b], cs_in.at[b],
            lambda j: (rows, slice(0, 128)), "z", z, "yh", yh, keep, finish)

    def reduce_diag(s):
        b, c0 = BUF[s], 128 * s

        @pl.loop(0, 4)
        def _(t):
            w = ls[s][pl.ds(4 * t, 4), :, :].reshape(256, KC[s])
            acc = nt(rh[:, c0:1280], w) + nt(rl[:, c0:1280], w)
            dp[b, 2 * t] = acc[:, 0:128]
            dp[b, 2 * t + 1] = acc[:, 128:256]

        started = []
        for k, (a, d) in enumerate(others):
            py, pz = lax.rem(yh + a, 2), lax.rem(z + d, 4)
            copy = remote(dp.at[b, py * 4 + pz], dl.at[b, k], {"yh": py, "z": pz})
            copy.start()
            started.append(copy)
        yield
        for copy in started:
            copy.wait_recv()
        v = diag[s] - dp[b, yh * 4 + z]
        for k in range(7):
            v = v - dl[b, k]
        df[s] = v
        if s > 0:
            hi, lo = split(v)
            kh[64 * (s - 1) : 64 * s, 128 * (s - 1) : 128 * s] = hi
            kl[64 * (s - 1) : 64 * s, 128 * (s - 1) : 128 * s] = lo
        to_out(df.at[s], out.at[s, :, s, :])
        for copy in started:
            copy.wait_send()
        yield

    def each_r(s, lo, hi, body):
        @pl.loop(lo, hi)
        def _(t):
            body(us[s][pl.ds(2 * t, 2), :, :].reshape(256, 640 - U0[s]),
                 lambda q: (BUF[s], q % 2, 2 * t + q // 2))

    def each_c(s, lo, hi, body):
        @pl.loop(lo, hi)
        def _(t):
            body(ls[s][pl.ds(4 * t, 4), :, :].reshape(256, KC[s]), BUF[s], 2 * t)

    def heavy_c(s, lo=0, hi=4):
        def body(w, b, r):
            w = w[:, 256 - 128 * s :]
            acc = nt(kh[128:640, 256:1280], w) + nt(kl[128:640, 256:1280], w)
            cp[b, r, 128:640, :] = acc[:, 0:128]
            cp[b, r + 1, 128:640, :] = acc[:, 128:256]

        each_c(s, lo, hi, body)

    def heavy_r(s, lo=0, hi=4):
        def body(w, block):
            w = w[:, 128 - U0[s] :]
            acc = nn(w, kh[128:640, 256:1280]) + nn(w, kl[128:640, 256:1280])
            for q in range(4):
                rp[(*block(q), slice(None), slice(256, 1280))] = acc[64 * q : 64 * (q + 1), :]

        each_r(s, lo, hi, body)

    def extra_r(s):
        def body(w, block):
            w = w[:, 0:128]
            acc = nn(w, kh[0:128, 256:1280]) + nn(w, kl[0:128, 256:1280])
            for q in range(4):
                rp[(*block(q), slice(None), slice(256, 1280))] += acc[64 * q : 64 * (q + 1), :]

        each_r(s, 0, 4, body)

    def extra_c(s):
        def body(w, b, r):
            w = w[:, 0 : 256 - 128 * s]
            at = slice(128 * s, 256)
            acc = nt(kh[128:640, at], w) + nt(kl[128:640, at], w)
            cp[b, r, 128:640, :] += acc[:, 0:128]
            cp[b, r + 1, 128:640, :] += acc[:, 128:256]

        each_c(s, 0, 4, body)

    def tail_r(s):
        def body(w, block):
            at = slice(128 * s, 256)
            acc = nn(w, kh[0:640, at]) + nn(w, kl[0:640, at])
            for q in range(4):
                rp[(*block(q), slice(None), at)] = acc[64 * q : 64 * (q + 1), :]

        each_r(s, 0, 4, body)

    def tail_c(s):
        def body(w, b, r):
            at = slice(64 * s, 128)
            acc = nt(kh[at, 128 * s : 1280], w) + nt(kl[at, 128 * s : 1280], w)
            cp[b, r, at, :] = acc[:, 0:128]
            cp[b, r + 1, at, :] = acc[:, 128:256]

        each_c(s, 0, 4, body)

    gl = {s: gather_l(s) for s in (2, 1, 0)}
    gu = {s: gather_u(s) for s in (2, 1, 0)}

    def step(name, gen):
        with jax.named_scope(name):
            next(gen)

    def step_gather(s):
        step(f"gl{s}", gl[s])
        step(f"gu{s}", gu[s])

    def run(name, f, *args):
        with jax.named_scope(name):
            f(*args)

    step_gather(2)
    with jax.named_scope("split"):
        for b in range(8):
            loads[b].wait()
            to_out(a32.at[b], out.at[3:11, :, 3 + b, :])
            hi, lo = split(a32[b].reshape(512, 128))
            kh[128:640, (b + 2) * 128 : (b + 3) * 128] = hi
            kl[128:640, (b + 2) * 128 : (b + 3) * 128] = lo
        for ref in (kh, kl):
            ref[0:128, :] = jnp.zeros((128, 1280), BF16)
            ref[128:640, 0:256] = jnp.zeros((512, 256), BF16)
    for _ in range(4):
        step_gather(2)
    step_gather(1)
    run("hr2", heavy_r, 2)
    run("hc2", heavy_c, 2)
    for s in (2, 1, 0):
        t = s - 1
        if t >= 0:
            after = [lambda: step_gather(t)] * 4
            after += [lambda: run(f"hr{t}", heavy_r, t), lambda: run(f"hc{t}", heavy_c, t)]
            if t == 1:
                after.append(lambda: step_gather(0))
        else:
            after = []

        def fill(count):
            for _ in range(count):
                if after:
                    after.pop(0)()

        r, c = reduce_rows(s), reduce_cols(s)
        step(f"r{s}", r)
        step(f"c{s}", c)
        fill(1)
        step(f"r{s}", r)
        step(f"c{s}", c)
        fill(1)
        step(f"r{s}", r)
        step(f"c{s}", c)
        fill(2)
        step(f"r{s}", r)
        step(f"c{s}", c)
        fill(1)
        step(f"r{s}", r)
        d = reduce_diag(s)
        step(f"d{s}", d)
        step(f"r{s}", r)
        fill(9)
        if t >= 0:
            run(f"xr{t}", extra_r, t)
            run(f"xc{t}", extra_c, t)
        step(f"d{s}", d)
        if t >= 0:
            run(f"tr{t}", tail_r, t)
            run(f"tc{t}", tail_c, t)
    for copy in out_copies:
        copy.wait()


def per_device(region, l_panels, u_panels, diag_inv, pattern):
    lin = l_panels[:, :, 1:, :].reshape(3, 64, 1280)
    uin = u_panels[:, 1:].transpose(0, 3, 1, 2).reshape(3, 128, 640)
    smem = pl.BlockSpec(memory_space=pltpu.SMEM)
    vmem = pl.BlockSpec(memory_space=pltpu.VMEM)
    hbm = pl.BlockSpec(memory_space=pl.ANY)
    sem = lambda n: pltpu.SemaphoreType.DMA((n,))
    return pl.pallas_call(
        kernel,
        name="selinv",
        out_shape=jax.ShapeDtypeStruct((NSEG, 64, NSEG, 128), F32),
        in_specs=[smem, hbm, vmem, vmem, vmem],
        out_specs=hbm,
        scratch_shapes=[
            pltpu.VMEM((8, 8, 64, 128), F32),
            pltpu.VMEM((640, 1280), BF16),
            pltpu.VMEM((640, 1280), BF16),
            pltpu.VMEM((16, 64, KC[2]), BF16),
            pltpu.VMEM((16, 64, KC[1]), BF16),
            pltpu.VMEM((16, 64, KC[0]), BF16),
            pltpu.VMEM((8, 128, 512), BF16),
            pltpu.VMEM((8, 128, 640), BF16),
            pltpu.VMEM((8, 128, 640), BF16),
            pltpu.VMEM((2, 8, 640, 128), F32),
            pltpu.VMEM((2, 2, 8, 64, 1280), F32),
            pltpu.VMEM((2, 8, 64, 1280), F32),
            pltpu.VMEM((2, 7, 64, 1280), I16),
            pltpu.VMEM((2, 7, 64, 1280), I16),
            pltpu.VMEM((2, 7, 8, 128), F32),
            pltpu.VMEM((2, 7, 8, 128), F32),
            pltpu.VMEM((2, 7, 640, 128), I16),
            pltpu.VMEM((2, 7, 640, 128), I16),
            pltpu.VMEM((2, 7, 8, 128), F32),
            pltpu.VMEM((2, 7, 8, 128), F32),
            pltpu.VMEM((2, 8, 64, 128), F32),
            pltpu.VMEM((2, 7, 64, 128), F32),
            pltpu.VMEM((3, 640, 128), F32),
            pltpu.VMEM((3, 64, 1280), F32),
            pltpu.VMEM((3, 64, 128), F32),
            pltpu.VMEM((64, 1280), BF16),
            pltpu.VMEM((64, 1280), BF16),
            sem(200),
            sem(200),
            sem(100),
        ],
        compiler_params=pltpu.CompilerParams(
            collective_id=0, has_side_effects=True, vmem_limit_bytes=64000 * 1024),
    )(pattern, region, lin, uin, diag_inv)


def solution(mesh):
    split_mesh = Mesh(mesh.devices.reshape(2, 4, 4, 2, 2), ROW + COL)
    in_specs = (
        P(None, COL, None, ROW),
        P(None, COL, None, ROW),
        P(None, None, COL, ROW),
        P(None, COL, ROW),
        P(),
    )
    out_specs = P(None, COL, None, ROW)
    return jax.shard_map(
        per_device, mesh=split_mesh, in_specs=in_specs, out_specs=out_specs, check_vma=False
    )
```

```python
import jax
import jax.numpy as jnp
from jax import lax
from jax.experimental import pallas as pl
from jax.experimental.pallas import tpu as pltpu
from jax.sharding import Mesh
from jax.sharding import PartitionSpec as P

F32 = jnp.float32
BF16 = jnp.bfloat16
I16 = jnp.int16
NSEG = 11
ROW = ("yh", "z")
COL = ("x", "yl", "core")
KC = {2: 1024, 1: 1152, 0: 1280}
U0 = {2: 128, 1: 0, 0: 0}
BUF = {2: 0, 1: 1, 0: 0}
PARTS = {"A": (2, 6), "B": (6, 10)}
TOP = 32700.0
PLAN = (
    "gu2 gl2 gl1 gu1",
    "S2 gu0 gl0 gu2",
    "gu2 H20 gl2 gl2",
    "k2 h20 k2 gl1",
    "gl1 gl2 gu2 H21",
    "H22 k2 h21 gu1",
    "gu1 h22 gu0 gu0",
    "gu2 gu2 H23 r2A",
    "gl1 r2B gl2 gl0",
    "gl0 gu1 r2A r2B",
    "gl2 h23 c2B c2A",
    "gl1 gl1 h11 gu0",
    "gu1 gu1 h10 r2A",
    "H11 H10 c2B r2B",
    "gl0 c2A r2A gu0",
    "gu0 r2B c2B r2A",
    "X1A r1A r2A c2A",
    "gl0 m2A r2B X1B",
    "r1B m2B c2B d2",
    "r1A x1B c1B r1B",
    "c2A x1A T1 t1",
    "r1A c1B d2 u1",
    "r1T c1A r1B r2B",
    "H01 H00 r1A c1B",
    "r1T gl0 c1A h01",
    "r1B h00 r1A r1A",
    "X0A r0A c1A c1T",
    "m1A c1B x0B c0B",
    "r0A r1T m1T r1B",
    "m1B d1 X0B r0B",
    "c1A x0A r0A r1T",
    "c1T T0 r0B c0A",
    "t0 r0A d1 u0",
    "c0T r1B c0B r0T",
    "r0B c0A r0T r0A",
    "r0A m0A r0B c0T",
    "c0B c0A r0T r0T",
    "r0B r0B m0B m0T",
    "d0 c0B c0A d0",
)
MESH = pl.DeviceIdType.MESH


def nt(a, b):
    return lax.dot_general(a, b, (((1,), (1,)), ((), ())), preferred_element_type=F32)


def nn(a, b):
    return lax.dot_general(a, b, (((1,), (0,)), ((), ())), preferred_element_type=F32)


def nt2(hi, lo, w):
    n = hi.shape[0]
    if hi.shape[1] <= 128:
        return nt(jnp.concatenate([hi, lo], axis=1), jnp.concatenate([w, w], axis=1))
    both = nt(jnp.concatenate([hi, lo], axis=0), w)
    return both[:n] + both[n:]


def nn2(w, hi, lo):
    n = hi.shape[1]
    if hi.shape[0] <= 128:
        return nn(jnp.concatenate([w, w], axis=1), jnp.concatenate([hi, lo], axis=0))
    if n <= 128:
        both = nn(w, jnp.concatenate([hi, lo], axis=1))
        return both[:, :n] + both[:, n:]
    return nn(w, hi) + nn(w, lo)


def split(v):
    hi = v.astype(BF16)
    return hi, (v - hi.astype(F32)).astype(BF16)


def pack(ref, v):
    v = v.reshape(-1, 8, 128)
    top = jnp.maximum(jnp.max(jnp.abs(v), axis=0), 1e-30)
    unit = jnp.ceil(jnp.log2(top * (1.0 / TOP)))
    ref[0:16, :] = jnp.concatenate([unit, unit], axis=0).astype(jnp.int32).astype(I16)
    q = jnp.round(v * jnp.exp2(-unit)).reshape(-1, 128)
    ref[16 : 16 + q.shape[0], :] = q.astype(jnp.int32).astype(I16)


def unpack(ref, tiles):
    unit = jnp.exp2(ref[0:16, :].astype(F32)[0:8])
    v = ref[16 : 16 + 64 * tiles, :].astype(F32)
    return (v.reshape(-1, 8, 128) * unit).reshape(tiles, 64, 128)


class Sems:
    def __init__(self, ref):
        self.ref, self.used = ref, 0

    def take(self):
        self.used += 1
        return self.ref.at[self.used - 1]


def kernel(pattern, reg, lin, uin, diag, out, a32, kh, kl, ls2, ls1, ls0, us2, us1, us0, cp, rp, rcl,
           rq_out, rq_in, cq_out, cq_in, dq_out, dq_in, tq_out, tq_in, vq_out, vq_in, dp, cf, rf, df, rh, rl, dkh, dkl,
           send_sem, recv_sem, out_sem):
    ls = {2: ls2, 1: ls1, 0: ls0}
    us = {2: us2, 1: us1, 0: us0}
    yh, z = lax.axis_index("yh"), lax.axis_index("z")
    x, yl, core = lax.axis_index("x"), lax.axis_index("yl"), lax.axis_index("core")
    sends, recvs, outs = Sems(send_sem), Sems(recv_sem), Sems(out_sem)
    out_copies = []

    def mask_row(s, i):
        return pattern[s, i + 1, x * 2 + yl].astype(F32)

    def mask_col(s, i):
        return pattern[s, i + 1, yh * 4 + z].astype(F32)

    def remote(src, dst, where):
        copy = pltpu.make_async_remote_copy(
            src_ref=src, dst_ref=dst, send_sem=sends.take(), recv_sem=recvs.take(),
            device_id=where, device_id_type=MESH)
        copy.start()
        return copy

    def to_out(src, dst):
        copy = pltpu.make_async_copy(src, dst, outs.take())
        copy.start()
        out_copies.append(copy)

    def ring(axis, here):
        places = [lax.rem(here + d, 4) for d in (1, 3, 2)]
        return (*places, {axis: places[0]}, {axis: places[1]})

    offsets = [(a, d) for a in range(2) for d in range(4) if (a, d) != (0, 0)]
    row_peers = [(lax.rem(yh + a, 2), lax.rem(z + d, 4)) for a, d in offsets]
    col_peers = [(lax.rem(yl + a, 2), lax.rem(x + d, 4)) for a, d in offsets]
    with jax.named_scope("signal"):
        barrier = pltpu.get_barrier_semaphore()
        peers = [{"core": 1 - core}]
        peers += [{"yh": a, "z": d} for a, d in row_peers]
        peers += [{"yl": a, "x": d} for a, d in col_peers]
        for peer in peers:
            pl.semaphore_signal(barrier, inc=1, device_id=peer, device_id_type=MESH)
    loads = [pltpu.make_async_copy(reg.at[:, :, b, :], a32.at[b], outs.take()) for b in range(8)]
    for copy in loads:
        copy.start()
    with jax.named_scope("own"):
        lane = lax.broadcasted_iota(jnp.int32, (128, 128), 1)
        for s in (2, 1, 0):
            for i in range(s, 10):
                v = lin[s, :, 128 * i : 128 * (i + 1)].astype(F32) * mask_col(s, i)
                ls[s][(x * 2 + yl) * 2 + core, :, 128 * (i - s) : 128 * (i - s + 1)] = v.astype(BF16)
            for i in range(U0[s] // 128, 5):
                m = jnp.where(lane < 64, mask_row(s, 2 * i), mask_row(s, 2 * i + 1))
                v = uin[s, :, 128 * i : 128 * (i + 1)].astype(F32) * m
                us[s][z * 2 + yh, :, 128 * i - U0[s] : 128 * (i + 1) - U0[s]] = v.astype(BF16)
    with jax.named_scope("barrier"):
        pl.semaphore_wait(barrier, len(peers))

    class Gather:
        def __init__(self, slab, axis, here, pair_axis, pair, to_core):
            self.args = (slab, axis, here, pair_axis, pair, to_core)
            self.started, self.crossed = [], []
            self.steps = self.run()

        def go(self, h, q, where):
            ref = self.args[0](h, q)
            copy = remote(ref, ref, where)
            self.started.append(copy)
            return copy

        def cross(self, h, q):
            if self.args[5]:
                self.crossed.append(self.go(h, q, {"core": 1 - core}))

        def wait_cross(self, count):
            for _ in range(count):
                self.crossed.pop(0).wait_recv()

        def run(self):
            _, axis, here, pair_axis, pair, _ = self.args
            hp, hm, h2, up, down = ring(axis, here)
            oq = 1 - pair
            m_pair = self.go(here, pair, {pair_axis: oq})
            m_op = self.go(here, pair, up)
            m_om = self.go(here, pair, down)
            self.cross(here, pair)
            yield
            m_pair.wait_recv()
            m_tp = self.go(here, oq, up)
            m_tm = self.go(here, oq, down)
            self.cross(here, oq)
            yield
            m_op.wait_recv()
            m_rp = self.go(hm, pair, up)
            self.cross(hm, pair)
            m_om.wait_recv()
            self.cross(hp, pair)
            yield
            m_tm.wait_recv()
            m_rm = self.go(hp, oq, down)
            self.cross(hp, oq)
            m_tp.wait_recv()
            self.cross(hm, oq)
            yield
            m_rp.wait_recv()
            self.cross(h2, pair)
            m_rm.wait_recv()
            self.cross(h2, oq)
            yield
            self.wait_cross(len(self.crossed))
            for copy in self.started:
                copy.wait_send()
            yield

    def gather_l(s):
        slab = ls[s]
        return Gather(lambda h, q: slab.at[(h * 2 + q) * 2 + core], "x", x, "yl", yl, True)

    def gather_u(s):
        slab = us[s]
        return Gather(lambda h, q: slab.at[h * 2 + q], "z", z, "yh", yh, False)

    def reduce_ring(val, q_out, q_in, tiles, axis, here, pair_axis, pair, keep, finish):
        hp, hm, h2, up, down = ring(axis, here)
        oq = 1 - pair
        started = []
        size = slice(0, 16 + 64 * tiles)

        def send(k, v, where):
            pack(q_out.at[k], v)
            copy = remote(q_out.at[k, size, :], q_in.at[k, size, :], where)
            started.append(copy)
            return copy

        def got(k):
            return unpack(q_in.at[k], tiles)

        m_rp = send(0, val(h2, 0), up)
        m_rm = send(1, val(h2, 1), down)
        m_ep = send(3, val(hp, 1), up)
        m_em = send(4, val(hm, 0), down)
        yield
        m_rp.wait_recv()
        m_fp = send(2, val(hp, 0) + got(0), up)
        m_rm.wait_recv()
        m_fm = send(5, val(hm, 1) + got(1), down)
        yield
        for copy in (m_ep, m_em, m_fp, m_fm):
            copy.wait_recv()
        m_y = send(6, val(here, oq) + got(2 + oq) + got(4 + oq), {pair_axis: oq})
        keep(val(here, pair) + got(2 + pair) + got(4 + pair))
        yield
        m_y.wait_recv()
        finish(got(6))
        for copy in started:
            copy.wait_send()
        yield

    def reduce_direct(val, q_out, q_in, tiles, places, finish):
        started = []
        size = slice(0, 16 + 64 * tiles)
        for k, (where, place) in enumerate(places):
            pack(q_out.at[k], val(place))
            started.append(remote(q_out.at[k, size, :], q_in.at[k, size, :], where))
        yield
        total = None
        for k, copy in enumerate(started):
            copy.wait_recv()
            v = unpack(q_in.at[k], tiles)
            total = v if total is None else total + v
        finish(total)
        for copy in started:
            copy.wait_send()
        yield

    row_places = [({"yh": a, "z": d}, a * 4 + d) for a, d in row_peers]
    col_places = [({"yl": a, "x": d}, d * 2 + a) for a, d in col_peers]

    def keep_row(s, i, v):
        rf[s, i] = v
        hi, lo = split(v)
        at = slice(128 * i, 128 * (i + 1))
        rh[:, at] = hi
        rl[:, at] = lo
        if s > 0:
            kh[64 * (s - 1) : 64 * s, at] = hi
            kl[64 * (s - 1) : 64 * s, at] = lo
        to_out(rf.at[s, i], out.at[s, :, i + 1, :])

    def keep_col(s, i, v):
        cf[s, i] = v
        if s > 0:
            hi, lo = split(v)
            kh[64 * i : 64 * (i + 1), 128 * (s - 1) : 128 * s] = hi
            kl[64 * i : 64 * (i + 1), 128 * (s - 1) : 128 * s] = lo

    def rows_part(s, part):
        b = BUF[s]
        lo, hi = PARTS.get(part, (s, 2))
        over = remote(rp.at[b, 1 - core, :, lo:hi], rcl.at[b, :, lo:hi], {"core": 1 - core})
        yield
        over.wait_recv()

        def val(place):
            return rp[b, core, place, lo:hi] + rcl[b, place, lo:hi]

        def keep(v):
            rf[s, lo:hi] = v

        def finish(last):
            for i in range(lo, hi):
                keep_row(s, i, -mask_col(s, i) * (rf[s, i] + last[i - lo]))

        if part == "T":
            keep(val(x * 2 + yl))
            yield from reduce_direct(val, tq_out.at[b], tq_in.at[b], hi - lo, col_places, finish)
        else:
            p = "AB".index(part)
            yield from reduce_ring(lambda h, q: val(h * 2 + q), rq_out.at[b, p], rq_in.at[b, p], hi - lo,
                                   "x", x, "yl", yl, keep, finish)
        over.wait_send()
        yield

    def cols_part(s, part):
        b = BUF[s]
        lo, hi = PARTS.get(part, (s, 2))

        def val(place):
            return cp[b, place, lo:hi]

        def keep(v):
            cf[s, lo:hi] = v

        def finish(last):
            for i in range(lo, hi):
                keep_col(s, i, -mask_row(s, i) * (cf[s, i] + last[i - lo]))
            to_out(cf.at[s, lo:hi], out.at[lo + 1 : hi + 1, :, s, :])

        if part == "T":
            keep(val(yh * 4 + z))
            yield from reduce_direct(val, vq_out.at[b], vq_in.at[b], hi - lo, row_places, finish)
        else:
            p = "AB".index(part)
            yield from reduce_ring(lambda h, q: val(q * 4 + h), cq_out.at[b, p], cq_in.at[b, p], hi - lo,
                                   "z", z, "yh", yh, keep, finish)

    def diag_terms(s, part):
        b = BUF[s]
        lo, hi = PARTS.get(part, (s, 2))

        @pl.loop(0, 4)
        def _(t):
            w = ls[s][pl.ds(4 * t, 4), :, 128 * (lo - s) : 128 * (hi - s)].reshape(256, 128 * (hi - lo))
            at = slice(128 * lo, 128 * hi)
            acc = nt2(rh[:, at], rl[:, at], w)
            for q in range(2):
                if part == "A":
                    dp[b, 2 * t + q] = acc[:, 128 * q : 128 * (q + 1)]
                else:
                    dp[b, 2 * t + q] += acc[:, 128 * q : 128 * (q + 1)]

    def reduce_diag(s):
        b = BUF[s]

        def finish(total):
            v = diag[s] - dp[b, yh * 4 + z] - total[0]
            df[s] = v
            if s > 0:
                at, cols = slice(64 * (s - 1), 64 * s), slice(128 * (s - 1), 128 * s)
                for k, dk, part in zip((kh, kl), (dkh, dkl), split(v)):
                    k[at, cols] = part
                    dk[...] = jnp.zeros((128, 128), BF16)
                    dk[at, :] = part
            to_out(df.at[s], out.at[s, :, s, :])

        yield from reduce_direct(lambda place: dp[b, place], dq_out.at[b], dq_in.at[b], 1, row_places, finish)

    def r_block(s, t, lo, hi, add, mul):
        b = BUF[s]
        acc = mul(us[s][pl.ds(2 * t, 2), :, :].reshape(256, 640 - U0[s]))
        for q in range(4):
            for i in range(lo, hi):
                v = acc[64 * q : 64 * (q + 1), 128 * (i - lo) : 128 * (i - lo + 1)]
                if add:
                    rp[b, q % 2, t + 4 * (q // 2), i] += v
                else:
                    rp[b, q % 2, t + 4 * (q // 2), i] = v

    def c_block(s, t, lo, hi, add, mul):
        b = BUF[s]
        acc = mul(ls[s][pl.ds(4 * t, 4), :, :].reshape(256, KC[s]))
        for q in range(2):
            for i in range(lo, hi):
                v = acc[64 * (i - lo) : 64 * (i - lo + 1), 128 * q : 128 * (q + 1)]
                if add:
                    cp[b, 2 * t + q, i] += v
                else:
                    cp[b, 2 * t + q, i] = v

    def heavy_c(s, t):
        def mul(w):
            w = w[:, 256 - 128 * s :]
            return nt2(kh[128:640, 256:1280], kl[128:640, 256:1280], w)

        c_block(s, t, 2, 10, False, mul)

    def heavy_r(s, t):
        def mul(w):
            w = w[:, 128 - U0[s] :]
            return nn(w, kh[128:640, 256:1280]) + nn(w, kl[128:640, 256:1280])

        r_block(s, t, 2, 10, False, mul)

    def extra_r(s, part):
        lo, hi = PARTS[part]
        at = slice(128 * lo, 128 * hi)

        @pl.loop(0, 4)
        def _(t):
            r_block(s, t, lo, hi, True, lambda w: nn2(w[:, 0:128], kh[0:128, at], kl[0:128, at]))

    def extra_c(s, part):
        lo, hi = PARTS[part]
        at, mid = slice(64 * lo, 64 * hi), slice(128 * s, 256)

        @pl.loop(0, 4)
        def _(t):
            c_block(s, t, lo, hi, True, lambda w: nt2(kh[at, mid], kl[at, mid], w[:, 0 : 256 - 128 * s]))


    def tail_r(s):
        at = slice(128 * s, 256)

        @pl.loop(0, 4)
        def _(t):
            r_block(s, t, s, 2, False, lambda w: nn2(w, kh[0:640, at], kl[0:640, at]))

    def tail_c(s):
        at, cols = slice(64 * s, 128), slice(128 * s, 1280)

        @pl.loop(0, 4)
        def _(t):
            c_block(s, t, s, 2, False, lambda w: nt2(kh[at, cols], kl[at, cols], w))

    def tail_diag(s):
        @pl.loop(0, 4)
        def _(t):
            at = slice(64 * s, 64 * (s + 1))
            r_block(s, t, s, s + 1, True, lambda w: nn2(w[:, 0:128], dkh[...], dkl[...]))
            c_block(s, t, s, s + 1, True, lambda w: nt2(dkh[at, :], dkl[at, :], w[:, 0:128]))

    gl = {s: gather_l(s) for s in (2, 1, 0)}
    gu = {s: gather_u(s) for s in (2, 1, 0)}

    def run(name, f, *args):
        with jax.named_scope(name):
            f(*args)

    def split_region():
        for b in range(8):
            loads[b].wait()
            to_out(a32.at[b], out.at[3:11, :, 3 + b, :])
            hi, lo = split(a32[b].reshape(512, 128))
            kh[128:640, (b + 2) * 128 : (b + 3) * 128] = hi
            kl[128:640, (b + 2) * 128 : (b + 3) * 128] = lo
        for ref in (kh, kl):
            ref[0:128, :] = jnp.zeros((128, 1280), BF16)
            ref[128:640, 0:256] = jnp.zeros((512, 256), BF16)

    places = {}
    for f, axis, here in ((heavy_r, "z", z), (heavy_c, "x", x)):
        up, down, far, *_ = ring(axis, here)
        places[f] = (here, up, down, far)

    def heavy(f, s, piece):
        if s == 2:
            f(s, places[f][piece])
        else:
            pl.loop(2 * piece, 2 * piece + 2)(lambda t: f(s, t))

    R = {(s, p): rows_part(s, p) for s in (2, 1, 0) for p in "ABT"}
    C = {(s, p): cols_part(s, p) for s in (2, 1, 0) for p in "ABT"}
    D = {s: reduce_diag(s) for s in (2, 1, 0)}
    actions = {
        "gl": lambda s, p: next(gl[s].steps),
        "gu": lambda s, p: next(gu[s].steps),
        "k": lambda s, p: gl[s].wait_cross(2),
        "S": lambda s, p: split_region(),
        "H": lambda s, p: heavy(heavy_r, s, int(p)),
        "h": lambda s, p: heavy(heavy_c, s, int(p)),
        "r": lambda s, p: next(R[s, p]),
        "c": lambda s, p: next(C[s, p]),
        "d": lambda s, p: next(D[s]),
        "X": extra_r,
        "x": extra_c,
        "m": diag_terms,
        "T": lambda s, p: tail_r(s),
        "t": lambda s, p: tail_c(s),
        "u": lambda s, p: tail_diag(s),
    }
    for name in " ".join(PLAN).split():
        kind = name[:2] if name[0] == "g" else name[0]
        rest = name[len(kind) :]
        run(name, actions[kind], int(rest[0]), rest[1:])
    for copy in out_copies:
        copy.wait()


def per_device(region, l_panels, u_panels, diag_inv, pattern):
    lin = l_panels[:, :, 1:, :].reshape(3, 64, 1280)
    uin = u_panels[:, 1:].transpose(0, 3, 1, 2).reshape(3, 128, 640)
    smem = pl.BlockSpec(memory_space=pltpu.SMEM)
    vmem = pl.BlockSpec(memory_space=pltpu.VMEM)
    hbm = pl.BlockSpec(memory_space=pl.ANY)
    sem = lambda n: pltpu.SemaphoreType.DMA((n,))
    return pl.pallas_call(
        kernel,
        name="selinv",
        out_shape=jax.ShapeDtypeStruct((NSEG, 64, NSEG, 128), F32),
        in_specs=[smem, hbm, vmem, vmem, vmem],
        out_specs=hbm,
        scratch_shapes=[
            pltpu.VMEM((8, 8, 64, 128), F32),
            pltpu.VMEM((640, 1280), BF16),
            pltpu.VMEM((640, 1280), BF16),
            pltpu.VMEM((16, 64, KC[2]), BF16),
            pltpu.VMEM((16, 64, KC[1]), BF16),
            pltpu.VMEM((16, 64, KC[0]), BF16),
            pltpu.VMEM((8, 128, 512), BF16),
            pltpu.VMEM((8, 128, 640), BF16),
            pltpu.VMEM((8, 128, 640), BF16),
            pltpu.VMEM((2, 8, 10, 64, 128), F32),
            pltpu.VMEM((2, 2, 8, 10, 64, 128), F32),
            pltpu.VMEM((2, 8, 10, 64, 128), F32),
            pltpu.VMEM((2, 2, 7, 272, 128), I16),
            pltpu.VMEM((2, 2, 7, 272, 128), I16),
            pltpu.VMEM((2, 2, 7, 272, 128), I16),
            pltpu.VMEM((2, 2, 7, 272, 128), I16),
            pltpu.VMEM((2, 7, 80, 128), I16),
            pltpu.VMEM((2, 7, 80, 128), I16),
            pltpu.VMEM((2, 7, 144, 128), I16),
            pltpu.VMEM((2, 7, 144, 128), I16),
            pltpu.VMEM((2, 7, 144, 128), I16),
            pltpu.VMEM((2, 7, 144, 128), I16),
            pltpu.VMEM((2, 8, 64, 128), F32),
            pltpu.VMEM((3, 10, 64, 128), F32),
            pltpu.VMEM((3, 10, 64, 128), F32),
            pltpu.VMEM((3, 64, 128), F32),
            pltpu.VMEM((64, 1280), BF16),
            pltpu.VMEM((64, 1280), BF16),
            pltpu.VMEM((128, 128), BF16),
            pltpu.VMEM((128, 128), BF16),
            sem(260),
            sem(260),
            sem(100),
        ],
        compiler_params=pltpu.CompilerParams(
            collective_id=0, has_side_effects=True, vmem_limit_bytes=64000 * 1024),
    )(pattern, region, lin, uin, diag_inv)


def solution(mesh):
    split_mesh = Mesh(mesh.devices.reshape(2, 4, 4, 2, 2), ROW + COL)
    in_specs = (
        P(None, COL, None, ROW),
        P(None, COL, None, ROW),
        P(None, None, COL, ROW),
        P(None, COL, ROW),
        P(),
    )
    out_specs = P(None, COL, None, ROW)
    return jax.shard_map(
        per_device, mesh=split_mesh, in_specs=in_specs, out_specs=out_specs, check_vma=False
    )
```

```python
import jax
import jax.numpy as jnp
from jax import lax
from jax.experimental import pallas as pl
from jax.experimental.pallas import tpu as pltpu
from jax.sharding import Mesh
from jax.sharding import PartitionSpec as P

F32 = jnp.float32
BF16 = jnp.bfloat16
I16 = jnp.int16
NSEG = 11
ROW = ("yh", "z")
COL = ("x", "yl", "core")
KC = {2: 1024, 1: 1152, 0: 1280}
U0 = {2: 128, 1: 0, 0: 0}
BUF = {2: 0, 1: 1, 0: 0}
PARTS = {"A": (2, 6), "B": (6, 10)}
TOP = 32700.0
SENDS, RECVS, OUTS = 61, 170, 35
PLAN = (
    "gu2 gl2 gl1 gu1",
    "S2 gu0 gl0 gu2",
    "gu2 H20 gl2 gl2",
    "k2 h20 k2 gl1",
    "gl1 gl2 gu2 H21",
    "H22 k2 h21 gu1",
    "gu1 h22 gu0 gu0",
    "gu2 gu2 H23 r2A",
    "gl1 r2B gl2 gl0",
    "gl0 gu1 r2A r2B",
    "gl2 h23 c2B c2A",
    "gl1 gl1 h11 gu0",
    "gu1 gu1 h10 r2A",
    "H11 H10 c2B r2B",
    "gl0 c2A r2A gu0",
    "gu0 r2B c2B r2A",
    "X1A r1A r2A c2A",
    "gl0 m2A r2B X1B",
    "r1B m2B c2B d2",
    "r1A x1B c1B r1B",
    "c2A x1A T1 t1",
    "r1A c1B d2 u1",
    "r1T c1A r1B r2B",
    "H01 H00 r1A c1B",
    "r1T gl0 c1A h01",
    "r1B h00 r1A r1A",
    "X0A r0A c1A c1T",
    "m1A c1B x0B c0B",
    "r0A r1T m1T r1B",
    "m1B d1 X0B r0B",
    "c1A x0A r0A r1T",
    "c1T T0 r0B c0A",
    "t0 r0A d1 u0",
    "c0T r1B c0B r0T",
    "r0B c0A r0T r0A",
    "r0A m0A r0B c0T",
    "c0B c0A r0T r0T",
    "r0B r0B m0B m0T",
    "d0 c0B c0A d0",
)
MESH = pl.DeviceIdType.MESH


def nt(a, b):
    return lax.dot_general(a, b, (((1,), (1,)), ((), ())), preferred_element_type=F32)


def nn(a, b):
    return lax.dot_general(a, b, (((1,), (0,)), ((), ())), preferred_element_type=F32)


def nt2(hi, lo, w):
    n = hi.shape[0]
    if hi.shape[1] <= 128:
        return nt(jnp.concatenate([hi, lo], axis=1), jnp.concatenate([w, w], axis=1))
    both = nt(jnp.concatenate([hi, lo], axis=0), w)
    return both[:n] + both[n:]


def nn2(w, hi, lo):
    n = hi.shape[1]
    if hi.shape[0] <= 128:
        return nn(jnp.concatenate([w, w], axis=1), jnp.concatenate([hi, lo], axis=0))
    if n <= 128:
        both = nn(w, jnp.concatenate([hi, lo], axis=1))
        return both[:, :n] + both[:, n:]
    return nn(w, hi) + nn(w, lo)


def split(v):
    hi = v.astype(BF16)
    return hi, (v - hi.astype(F32)).astype(BF16)


def pack(ref, v):
    v = v.reshape(-1, 8, 128)
    top = jnp.maximum(jnp.max(jnp.abs(v), axis=0), 1e-30)
    unit = jnp.ceil(jnp.log2(top * (1.0 / TOP)))
    ref[0:16, :] = jnp.concatenate([unit, unit], axis=0).astype(jnp.int32).astype(I16)
    q = jnp.round(v * jnp.exp2(-unit)).reshape(-1, 128)
    ref[16 : 16 + q.shape[0], :] = q.astype(jnp.int32).astype(I16)


def unpack(ref, tiles):
    unit = jnp.exp2(ref[0:16, :].astype(F32)[0:8])
    v = ref[16 : 16 + 64 * tiles, :].astype(F32)
    return (v.reshape(-1, 8, 128) * unit).reshape(tiles, 64, 128)


class Sems:
    def __init__(self, ref):
        self.ref, self.used, self.free = ref, 0, []

    def take(self):
        if self.free:
            return self.free.pop()
        self.used += 1
        return self.ref.at[self.used - 1]


def kernel(pattern, reg, lin, uin, diag, out, a32, kh, kl, ls2, ls1, ls0, us2, us1, us0, cp, rp, rcl,
           rq_out, rq_in, cq_out, cq_in, dq_out, dq_in, tq_out, tq_in, vq_out, vq_in, dp, cf, rf, df, rh, rl, dkh, dkl,
           send_sem, recv_sem, out_sem):
    ls = {2: ls2, 1: ls1, 0: ls0}
    us = {2: us2, 1: us1, 0: us0}
    yh, z = lax.axis_index("yh"), lax.axis_index("z")
    x, yl, core = lax.axis_index("x"), lax.axis_index("yl"), lax.axis_index("core")
    sends, recvs, outs = Sems(send_sem), Sems(recv_sem), Sems(out_sem)
    out_copies, send_sems, arrivals = [], {}, {}

    def mask_row(s, i):
        return pattern[s, x * 2 + yl, i + 1].astype(F32)

    def mask_col(s, i):
        return pattern[s, yh * 4 + z, i + 1].astype(F32)

    def remote(src, dst, where, key=None):
        sem = sends.take()
        if key is None or key not in arrivals:
            arrivals[key] = recvs.take()
        copy = pltpu.make_async_remote_copy(
            src_ref=src, dst_ref=dst, send_sem=sem, recv_sem=arrivals[key],
            device_id=where, device_id_type=MESH)
        copy.start()
        send_sems[id(copy)] = (copy, sem)
        return copy

    def sent(*copies):
        for copy in copies:
            copy.wait_send()
            sends.free.append(send_sems.pop(id(copy))[1])

    def to_out(src, dst):
        copy = pltpu.make_async_copy(src, dst, outs.take())
        copy.start()
        out_copies.append(copy)

    def ring(axis, here):
        places = [lax.rem(here + d, 4) for d in (1, 3, 2)]
        return (*places, {axis: places[0]}, {axis: places[1]})

    offsets = [(a, d) for a in range(2) for d in range(4) if (a, d) != (0, 0)]
    row_peers = [(lax.rem(yh + a, 2), lax.rem(z + d, 4)) for a, d in offsets]
    col_peers = [(lax.rem(yl + a, 2), lax.rem(x + d, 4)) for a, d in offsets]
    with jax.named_scope("signal"):
        barrier = pltpu.get_barrier_semaphore()
        peers = [{"core": 1 - core}]
        peers += [{"yh": a, "z": d} for a, d in row_peers]
        peers += [{"yl": a, "x": d} for a, d in col_peers]
        for peer in peers:
            pl.semaphore_signal(barrier, inc=1, device_id=peer, device_id_type=MESH)
    loads = [pltpu.make_async_copy(reg.at[:, :, b, :], a32.at[b], outs.take()) for b in range(8)]
    for copy in loads:
        copy.start()
    with jax.named_scope("own"):
        for s in (2, 1, 0):
            for i in range(s, 10):
                v = lin[s, i + 1].astype(F32) * mask_col(s, i)
                ls[s][(x * 2 + yl) * 2 + core, :, 128 * (i - s) : 128 * (i - s + 1)] = v.astype(BF16)
            for i in range(U0[s] // 64, 10, 2):
                pair = [uin[s, k + 1].astype(F32) * mask_row(s, k) for k in (i, i + 1)]
                v = jnp.concatenate(pair, axis=0).T
                us[s][z * 2 + yh, :, 64 * i - U0[s] : 64 * i + 128 - U0[s]] = v.astype(BF16)
    with jax.named_scope("barrier"):
        pl.semaphore_wait(barrier, len(peers))

    class Gather:
        def __init__(self, slab, axis, here, pair_axis, pair, to_core):
            self.args = (slab, axis, here, pair_axis, pair, to_core)
            self.started, self.crossed = [], []
            self.steps = self.run()

        def go(self, h, q, where):
            ref = self.args[0](h, q)
            copy = remote(ref, ref, where)
            self.started.append(copy)
            return copy

        def cross(self, h, q):
            if self.args[5]:
                self.crossed.append(self.go(h, q, {"core": 1 - core}))

        def wait_cross(self, count):
            for _ in range(count):
                self.crossed.pop(0).wait_recv()

        def run(self):
            _, axis, here, pair_axis, pair, _ = self.args
            hp, hm, h2, up, down = ring(axis, here)
            oq = 1 - pair
            m_pair = self.go(here, pair, {pair_axis: oq})
            m_op = self.go(here, pair, up)
            m_om = self.go(here, pair, down)
            self.cross(here, pair)
            yield
            m_pair.wait_recv()
            m_tp = self.go(here, oq, up)
            m_tm = self.go(here, oq, down)
            self.cross(here, oq)
            yield
            m_op.wait_recv()
            m_rp = self.go(hm, pair, up)
            self.cross(hm, pair)
            m_om.wait_recv()
            self.cross(hp, pair)
            yield
            m_tm.wait_recv()
            m_rm = self.go(hp, oq, down)
            self.cross(hp, oq)
            m_tp.wait_recv()
            self.cross(hm, oq)
            yield
            m_rp.wait_recv()
            self.cross(h2, pair)
            m_rm.wait_recv()
            self.cross(h2, oq)
            yield
            self.wait_cross(len(self.crossed))
            sent(*self.started)
            yield

    def gather_l(s):
        slab = ls[s]
        return Gather(lambda h, q: slab.at[(h * 2 + q) * 2 + core], "x", x, "yl", yl, True)

    def gather_u(s):
        slab = us[s]
        return Gather(lambda h, q: slab.at[h * 2 + q], "z", z, "yh", yh, False)

    def reduce_ring(key, val, q_out, q_in, tiles, axis, here, pair_axis, pair, keep, finish):
        hp, hm, h2, up, down = ring(axis, here)
        oq = 1 - pair
        started = []
        size = slice(0, 16 + 64 * tiles)

        def send(k, v, where):
            pack(q_out.at[k], v)
            copy = remote(q_out.at[k, size, :], q_in.at[k, size, :], where, (*key, k))
            started.append(copy)
            return copy

        def got(k):
            return unpack(q_in.at[k], tiles)

        m_rp = send(0, val(h2, 0), up)
        m_rm = send(1, val(h2, 1), down)
        m_ep = send(3, val(hp, 1), up)
        m_em = send(4, val(hm, 0), down)
        yield
        m_rp.wait_recv()
        m_fp = send(2, val(hp, 0) + got(0), up)
        m_rm.wait_recv()
        m_fm = send(5, val(hm, 1) + got(1), down)
        yield
        for copy in (m_ep, m_em, m_fp, m_fm):
            copy.wait_recv()
        m_y = send(6, val(here, oq) + got(2 + oq) + got(4 + oq), {pair_axis: oq})
        keep(val(here, pair) + got(2 + pair) + got(4 + pair))
        yield
        m_y.wait_recv()
        finish(got(6))
        sent(*started)
        yield

    def reduce_direct(key, val, q_out, q_in, tiles, places, finish):
        started = []
        size = slice(0, 16 + 64 * tiles)
        for k, (where, place) in enumerate(places):
            pack(q_out.at[k], val(place))
            started.append(remote(q_out.at[k, size, :], q_in.at[k, size, :], where, (*key, k)))
        yield
        total = None
        for k, copy in enumerate(started):
            copy.wait_recv()
            v = unpack(q_in.at[k], tiles)
            total = v if total is None else total + v
        finish(total)
        sent(*started)
        yield

    row_places = [({"yh": a, "z": d}, a * 4 + d) for a, d in row_peers]
    col_places = [({"yl": a, "x": d}, d * 2 + a) for a, d in col_peers]

    def keep_row(s, i, v):
        rf[s, i] = v
        hi, lo = split(v)
        at = slice(128 * i, 128 * (i + 1))
        rh[:, at] = hi
        rl[:, at] = lo
        if s > 0:
            kh[64 * (s - 1) : 64 * s, at] = hi
            kl[64 * (s - 1) : 64 * s, at] = lo

    def keep_col(s, i, v):
        cf[s, i] = v
        if s > 0:
            hi, lo = split(v)
            kh[64 * i : 64 * (i + 1), 128 * (s - 1) : 128 * s] = hi
            kl[64 * i : 64 * (i + 1), 128 * (s - 1) : 128 * s] = lo

    def rows_part(s, part):
        b = BUF[s]
        lo, hi = PARTS.get(part, (s, 2))
        over = remote(rp.at[b, 1 - core, :, lo:hi], rcl.at[b, :, lo:hi], {"core": 1 - core},
                      ("over", b, part))
        yield
        over.wait_recv()

        def val(place):
            return rp[b, core, place, lo:hi] + rcl[b, place, lo:hi]

        def keep(v):
            rf[s, lo:hi] = v

        def finish(last):
            for i in range(lo, hi):
                keep_row(s, i, -mask_col(s, i) * (rf[s, i] + last[i - lo]))
            to_out(rf.at[s, lo:hi], out.at[s, lo + 1 : hi + 1])

        if part == "T":
            keep(val(x * 2 + yl))
            yield from reduce_direct(("rT", b), val, tq_out.at[b], tq_in.at[b], hi - lo, col_places, finish)
        else:
            p = "AB".index(part)
            yield from reduce_ring(("r", b, p), lambda h, q: val(h * 2 + q), rq_out.at[b, p], rq_in.at[b, p], hi - lo,
                                   "x", x, "yl", yl, keep, finish)
        sent(over)
        yield

    def cols_part(s, part):
        b = BUF[s]
        lo, hi = PARTS.get(part, (s, 2))

        def val(place):
            return cp[b, place, lo:hi]

        def keep(v):
            cf[s, lo:hi] = v

        def finish(last):
            for i in range(lo, hi):
                keep_col(s, i, -mask_row(s, i) * (cf[s, i] + last[i - lo]))
            to_out(cf.at[s, lo:hi], out.at[lo + 1 : hi + 1, s])

        if part == "T":
            keep(val(yh * 4 + z))
            yield from reduce_direct(("cT", b), val, vq_out.at[b], vq_in.at[b], hi - lo, row_places, finish)
        else:
            p = "AB".index(part)
            yield from reduce_ring(("c", b, p), lambda h, q: val(q * 4 + h), cq_out.at[b, p], cq_in.at[b, p], hi - lo,
                                   "z", z, "yh", yh, keep, finish)

    def diag_terms(s, part):
        b = BUF[s]
        lo, hi = PARTS.get(part, (s, 2))

        @pl.loop(0, 4)
        def _(t):
            w = ls[s][pl.ds(4 * t, 4), :, 128 * (lo - s) : 128 * (hi - s)].reshape(256, 128 * (hi - lo))
            at = slice(128 * lo, 128 * hi)
            acc = nt2(rh[:, at], rl[:, at], w)
            for q in range(2):
                if part == "A":
                    dp[b, 2 * t + q] = acc[:, 128 * q : 128 * (q + 1)]
                else:
                    dp[b, 2 * t + q] += acc[:, 128 * q : 128 * (q + 1)]

    def reduce_diag(s):
        b = BUF[s]

        def finish(total):
            v = diag[s] - dp[b, yh * 4 + z] - total[0]
            df[s] = v
            if s > 0:
                at, cols = slice(64 * (s - 1), 64 * s), slice(128 * (s - 1), 128 * s)
                for k, dk, part in zip((kh, kl), (dkh, dkl), split(v)):
                    k[at, cols] = part
                    dk[...] = jnp.zeros((128, 128), BF16)
                    dk[at, :] = part
            to_out(df.at[s], out.at[s, s])

        yield from reduce_direct(("d", b), lambda place: dp[b, place], dq_out.at[b], dq_in.at[b], 1, row_places, finish)

    def r_block(s, t, lo, hi, add, mul):
        b = BUF[s]
        acc = mul(us[s][pl.ds(2 * t, 2), :, :].reshape(256, 640 - U0[s]))
        for q in range(4):
            for i in range(lo, hi):
                v = acc[64 * q : 64 * (q + 1), 128 * (i - lo) : 128 * (i - lo + 1)]
                if add:
                    rp[b, q % 2, t + 4 * (q // 2), i] += v
                else:
                    rp[b, q % 2, t + 4 * (q // 2), i] = v

    def c_block(s, t, lo, hi, add, mul):
        b = BUF[s]
        acc = mul(ls[s][pl.ds(4 * t, 4), :, :].reshape(256, KC[s]))
        for q in range(2):
            for i in range(lo, hi):
                v = acc[64 * (i - lo) : 64 * (i - lo + 1), 128 * q : 128 * (q + 1)]
                if add:
                    cp[b, 2 * t + q, i] += v
                else:
                    cp[b, 2 * t + q, i] = v

    def heavy_c(s, t):
        def mul(w):
            w = w[:, 256 - 128 * s :]
            return nt2(kh[128:640, 256:1280], kl[128:640, 256:1280], w)

        c_block(s, t, 2, 10, False, mul)

    def heavy_r(s, t):
        def mul(w):
            w = w[:, 128 - U0[s] :]
            return nn(w, kh[128:640, 256:1280]) + nn(w, kl[128:640, 256:1280])

        r_block(s, t, 2, 10, False, mul)

    def extra_r(s, part):
        lo, hi = PARTS[part]
        at = slice(128 * lo, 128 * hi)

        @pl.loop(0, 4)
        def _(t):
            r_block(s, t, lo, hi, True, lambda w: nn2(w[:, 0:128], kh[0:128, at], kl[0:128, at]))

    def extra_c(s, part):
        lo, hi = PARTS[part]
        at, mid = slice(64 * lo, 64 * hi), slice(128 * s, 256)

        @pl.loop(0, 4)
        def _(t):
            c_block(s, t, lo, hi, True, lambda w: nt2(kh[at, mid], kl[at, mid], w[:, 0 : 256 - 128 * s]))


    def tail_r(s):
        at = slice(128 * s, 256)

        @pl.loop(0, 4)
        def _(t):
            r_block(s, t, s, 2, False, lambda w: nn2(w, kh[0:640, at], kl[0:640, at]))

    def tail_c(s):
        at, cols = slice(64 * s, 128), slice(128 * s, 1280)

        @pl.loop(0, 4)
        def _(t):
            c_block(s, t, s, 2, False, lambda w: nt2(kh[at, cols], kl[at, cols], w))

    def tail_diag(s):
        @pl.loop(0, 4)
        def _(t):
            at = slice(64 * s, 64 * (s + 1))
            r_block(s, t, s, s + 1, True, lambda w: nn2(w[:, 0:128], dkh[...], dkl[...]))
            c_block(s, t, s, s + 1, True, lambda w: nt2(dkh[at, :], dkl[at, :], w[:, 0:128]))

    gl = {s: gather_l(s) for s in (2, 1, 0)}
    gu = {s: gather_u(s) for s in (2, 1, 0)}

    def run(name, f, *args):
        with jax.named_scope(name):
            f(*args)

    def split_region():
        for b in range(8):
            loads[b].wait()
            to_out(a32.at[b], out.at[3:11, 3 + b])
            hi, lo = split(a32[b].reshape(512, 128))
            kh[128:640, (b + 2) * 128 : (b + 3) * 128] = hi
            kl[128:640, (b + 2) * 128 : (b + 3) * 128] = lo
        for ref in (kh, kl):
            ref[0:128, :] = jnp.zeros((128, 1280), BF16)
            ref[128:640, 0:256] = jnp.zeros((512, 256), BF16)

    places = {}
    for f, axis, here in ((heavy_r, "z", z), (heavy_c, "x", x)):
        up, down, far, *_ = ring(axis, here)
        places[f] = (here, up, down, far)

    def heavy(f, s, piece):
        if s == 2:
            f(s, places[f][piece])
        else:
            pl.loop(2 * piece, 2 * piece + 2)(lambda t: f(s, t))

    R = {(s, p): rows_part(s, p) for s in (2, 1, 0) for p in "ABT"}
    C = {(s, p): cols_part(s, p) for s in (2, 1, 0) for p in "ABT"}
    D = {s: reduce_diag(s) for s in (2, 1, 0)}
    actions = {
        "gl": lambda s, p: next(gl[s].steps),
        "gu": lambda s, p: next(gu[s].steps),
        "k": lambda s, p: gl[s].wait_cross(2),
        "S": lambda s, p: split_region(),
        "H": lambda s, p: heavy(heavy_r, s, int(p)),
        "h": lambda s, p: heavy(heavy_c, s, int(p)),
        "r": lambda s, p: next(R[s, p]),
        "c": lambda s, p: next(C[s, p]),
        "d": lambda s, p: next(D[s]),
        "X": extra_r,
        "x": extra_c,
        "m": diag_terms,
        "T": lambda s, p: tail_r(s),
        "t": lambda s, p: tail_c(s),
        "u": lambda s, p: tail_diag(s),
    }
    for name in " ".join(PLAN).split():
        kind = name[:2] if name[0] == "g" else name[0]
        rest = name[len(kind) :]
        run(name, actions[kind], int(rest[0]), rest[1:])
    with jax.named_scope("outs"):
        for copy in out_copies:
            copy.wait()


def per_device(region, l_panels, u_panels, diag_inv, pattern):
    lin = l_panels.transpose(0, 2, 1, 3)
    blocks = pattern.transpose(0, 2, 1)
    smem = pl.BlockSpec(memory_space=pltpu.SMEM)
    vmem = pl.BlockSpec(memory_space=pltpu.VMEM)
    hbm = pl.BlockSpec(memory_space=pl.ANY)
    sem = lambda n: pltpu.SemaphoreType.DMA((n,))
    blocks_out = pl.pallas_call(
        kernel,
        name="selinv",
        out_shape=jax.ShapeDtypeStruct((NSEG, NSEG, 64, 128), F32),
        in_specs=[smem, hbm, vmem, vmem, vmem],
        out_specs=hbm,
        scratch_shapes=[
            pltpu.VMEM((8, 8, 64, 128), F32),
            pltpu.VMEM((640, 1280), BF16),
            pltpu.VMEM((640, 1280), BF16),
            pltpu.VMEM((16, 64, KC[2]), BF16),
            pltpu.VMEM((16, 64, KC[1]), BF16),
            pltpu.VMEM((16, 64, KC[0]), BF16),
            pltpu.VMEM((8, 128, 512), BF16),
            pltpu.VMEM((8, 128, 640), BF16),
            pltpu.VMEM((8, 128, 640), BF16),
            pltpu.VMEM((2, 8, 10, 64, 128), F32),
            pltpu.VMEM((2, 2, 8, 10, 64, 128), F32),
            pltpu.VMEM((2, 8, 10, 64, 128), F32),
            pltpu.VMEM((2, 2, 7, 272, 128), I16),
            pltpu.VMEM((2, 2, 7, 272, 128), I16),
            pltpu.VMEM((2, 2, 7, 272, 128), I16),
            pltpu.VMEM((2, 2, 7, 272, 128), I16),
            pltpu.VMEM((2, 7, 80, 128), I16),
            pltpu.VMEM((2, 7, 80, 128), I16),
            pltpu.VMEM((2, 7, 144, 128), I16),
            pltpu.VMEM((2, 7, 144, 128), I16),
            pltpu.VMEM((2, 7, 144, 128), I16),
            pltpu.VMEM((2, 7, 144, 128), I16),
            pltpu.VMEM((2, 8, 64, 128), F32),
            pltpu.VMEM((3, 10, 64, 128), F32),
            pltpu.VMEM((3, 10, 64, 128), F32),
            pltpu.VMEM((3, 64, 128), F32),
            pltpu.VMEM((64, 1280), BF16),
            pltpu.VMEM((64, 1280), BF16),
            pltpu.VMEM((128, 128), BF16),
            pltpu.VMEM((128, 128), BF16),
            sem(SENDS),
            sem(RECVS),
            sem(OUTS),
        ],
        compiler_params=pltpu.CompilerParams(
            collective_id=0, has_side_effects=True, vmem_limit_bytes=64000 * 1024),
    )(blocks, region, lin, u_panels, diag_inv)
    return blocks_out.transpose(0, 2, 1, 3)


def solution(mesh):
    split_mesh = Mesh(mesh.devices.reshape(2, 4, 4, 2, 2), ROW + COL)
    in_specs = (
        P(None, COL, None, ROW),
        P(None, COL, None, ROW),
        P(None, None, COL, ROW),
        P(None, COL, ROW),
        P(),
    )
    out_specs = P(None, COL, None, ROW)
    return jax.shard_map(
        per_device, mesh=split_mesh, in_specs=in_specs, out_specs=out_specs, check_vma=False
    )
```

```python
import jax
import jax.numpy as jnp
from jax import lax
from jax.experimental import pallas as pl
from jax.experimental.pallas import tpu as pltpu
from jax.sharding import Mesh
from jax.sharding import PartitionSpec as P

F32 = jnp.float32
BF16 = jnp.bfloat16
I16 = jnp.int16
NSEG = 11
ROW = ("yh", "z")
COL = ("x", "yl", "core")
KC = {2: 1024, 1: 1152, 0: 1280}
U0 = {2: 128, 1: 0, 0: 0}
BUF = {2: 0, 1: 1, 0: 0}
PARTS = {"A": (2, 6), "B": (6, 10)}
TOP = 32700.0
SENDS, RECVS, OUTS = 61, 170, 39
PLAN = (
    "gu2 gl2 gl1 gu1",
    "gu0 gl0 S2 gu2",
    "H20 gu2 gl2 gl2",
    "k2 h20 k2 gl1",
    "gl1 gl2 gu2 H21",
    "gu1 gu1 H22 k2",
    "h22 h21 gu0 gu0",
    "gu2 H23 gl1 r2A",
    "r2B gl2 gl0 gl0",
    "gu2 gu1 r2A r2B",
    "gl2 gl1 h23 c2B",
    "c2A gl1 h11 h10",
    "gu0 gu1 gu1 H11",
    "r2A H10 c2B r2B",
    "gl0 c2A r2A r2B",
    "gu0 gu0 c2B r2A",
    "X1A gl0 r2A c2A",
    "r2B r1A m2A m2B",
    "gl0 d2 X1B r1A",
    "r1B c2B x1B c2A",
    "c1B t1 r1B x1A",
    "c1A r1A T1 d2",
    "u1 c1T r1T r1B",
    "c1B r2B H00 c1A",
    "r1T h00 r1A H01",
    "c1T r1B h01 c1A",
    "c1B r1T r1A r1A",
    "X0A r0A m1A r1B",
    "r1B m1B m1T d1",
    "r0A c1A X0B r0B",
    "x0A c0A c1B T0",
    "r0A r0B t0 d1",
    "u0 c0T c0A x0B",
    "r0A r0T c0B r1T",
    "r0B r0T r0B c0T",
    "c0A r0A r0A m0A",
    "c0B r0T r0B r0B",
    "m0T c0B r0T m0B",
    "d0 c0A c0B d0",
)
MESH = pl.DeviceIdType.MESH


def nt(a, b):
    return lax.dot_general(a, b, (((1,), (1,)), ((), ())), preferred_element_type=F32)


def nn(a, b):
    return lax.dot_general(a, b, (((1,), (0,)), ((), ())), preferred_element_type=F32)


def nt2(hi, lo, w):
    n = hi.shape[0]
    if hi.shape[1] <= 128:
        return nt(jnp.concatenate([hi, lo], axis=1), jnp.concatenate([w, w], axis=1))
    both = nt(jnp.concatenate([hi, lo], axis=0), w)
    return both[:n] + both[n:]


def nn2(w, hi, lo):
    n = hi.shape[1]
    if hi.shape[0] <= 128:
        return nn(jnp.concatenate([w, w], axis=1), jnp.concatenate([hi, lo], axis=0))
    if n <= 128:
        both = nn(w, jnp.concatenate([hi, lo], axis=1))
        return both[:, :n] + both[:, n:]
    return nn(w, hi) + nn(w, lo)


def split(v):
    hi = v.astype(BF16)
    return hi, (v - hi.astype(F32)).astype(BF16)


def pack(ref, v):
    v = v.reshape(-1, 8, 128)
    top = jnp.maximum(jnp.max(jnp.abs(v), axis=0), 1e-30)
    unit = jnp.ceil(jnp.log2(top * (1.0 / TOP)))
    ref[0:16, :] = jnp.concatenate([unit, unit], axis=0).astype(jnp.int32).astype(I16)
    q = jnp.round(v * jnp.exp2(-unit)).reshape(-1, 128)
    ref[16 : 16 + q.shape[0], :] = q.astype(jnp.int32).astype(I16)


def unpack(ref, tiles):
    unit = jnp.exp2(ref[0:16, :].astype(F32)[0:8])
    v = ref[16 : 16 + 64 * tiles, :].astype(F32)
    return (v.reshape(-1, 8, 128) * unit).reshape(tiles, 64, 128)


class Sems:
    def __init__(self, ref):
        self.ref, self.used, self.free = ref, 0, []

    def take(self):
        if self.free:
            return self.free.pop()
        self.used += 1
        return self.ref.at[self.used - 1]


def kernel(pattern_in, reg, lin_in, uin_in, diag_in, out, pattern, lin, uin, diag, a32, kh, kl, ls2, ls1, ls0, us2, us1, us0, cp, rp, rcl,
           rq_out, rq_in, cq_out, cq_in, dq_out, dq_in, tq_out, tq_in, vq_out, vq_in, dp, cf, rf, df, rh, rl, dkh, dkl,
           send_sem, recv_sem, out_sem):
    ls = {2: ls2, 1: ls1, 0: ls0}
    us = {2: us2, 1: us1, 0: us0}
    yh, z = lax.axis_index("yh"), lax.axis_index("z")
    x, yl, core = lax.axis_index("x"), lax.axis_index("yl"), lax.axis_index("core")
    sends, recvs, outs = Sems(send_sem), Sems(recv_sem), Sems(out_sem)
    out_copies, send_sems, arrivals = [], {}, {}

    def mask_row(s, i):
        return pattern[s, x * 2 + yl, i + 1].astype(F32)

    def mask_col(s, i):
        return pattern[s, yh * 4 + z, i + 1].astype(F32)

    def remote(src, dst, where, key=None):
        sem = sends.take()
        if key is None or key not in arrivals:
            arrivals[key] = recvs.take()
        copy = pltpu.make_async_remote_copy(
            src_ref=src, dst_ref=dst, send_sem=sem, recv_sem=arrivals[key],
            device_id=where, device_id_type=MESH)
        copy.start()
        send_sems[id(copy)] = (copy, sem)
        return copy

    def sent(*copies):
        for copy in copies:
            copy.wait_send()
            sends.free.append(send_sems.pop(id(copy))[1])

    def to_out(src, dst):
        copy = pltpu.make_async_copy(src, dst, outs.take())
        copy.start()
        out_copies.append(copy)

    def ring(axis, here):
        places = [lax.rem(here + d, 4) for d in (1, 3, 2)]
        return (*places, {axis: places[0]}, {axis: places[1]})

    offsets = [(a, d) for a in range(2) for d in range(4) if (a, d) != (0, 0)]
    row_peers = [(lax.rem(yh + a, 2), lax.rem(z + d, 4)) for a, d in offsets]
    col_peers = [(lax.rem(yl + a, 2), lax.rem(x + d, 4)) for a, d in offsets]
    with jax.named_scope("signal"):
        barrier = pltpu.get_barrier_semaphore()
        peers = [{"core": 1 - core}]
        peers += [{"yh": a, "z": d} for a, d in row_peers]
        peers += [{"yl": a, "x": d} for a, d in col_peers]
        for peer in peers:
            pl.semaphore_signal(barrier, inc=1, device_id=peer, device_id_type=MESH)
    inputs = [pltpu.make_async_copy(src, dst, outs.take()) for src, dst in (
        (pattern_in, pattern), (lin_in, lin), (uin_in, uin), (diag_in, diag))]
    for copy in inputs:
        copy.start()
    loads = [pltpu.make_async_copy(reg.at[:, :, b, :], a32.at[b], outs.take()) for b in range(8)]
    for copy in loads:
        copy.start()
    for copy in inputs:
        copy.wait()
    with jax.named_scope("own"):
        for s in (2, 1, 0):
            for i in range(s, 10):
                v = lin[s, i + 1].astype(F32) * mask_col(s, i)
                ls[s][(x * 2 + yl) * 2 + core, :, 128 * (i - s) : 128 * (i - s + 1)] = v.astype(BF16)
            for i in range(U0[s] // 64, 10, 2):
                pair = [uin[s, k + 1].astype(F32) * mask_row(s, k) for k in (i, i + 1)]
                v = jnp.concatenate(pair, axis=0).T
                us[s][z * 2 + yh, :, 64 * i - U0[s] : 64 * i + 128 - U0[s]] = v.astype(BF16)
    with jax.named_scope("barrier"):
        pl.semaphore_wait(barrier, len(peers))

    class Gather:
        def __init__(self, slab, axis, here, pair_axis, pair, to_core):
            self.args = (slab, axis, here, pair_axis, pair, to_core)
            self.started, self.crossed = [], []
            self.steps = self.run()

        def go(self, h, q, where):
            ref = self.args[0](h, q)
            copy = remote(ref, ref, where)
            self.started.append(copy)
            return copy

        def cross(self, h, q):
            if self.args[5]:
                self.crossed.append(self.go(h, q, {"core": 1 - core}))

        def wait_cross(self, count):
            for _ in range(count):
                self.crossed.pop(0).wait_recv()

        def run(self):
            _, axis, here, pair_axis, pair, _ = self.args
            hp, hm, h2, up, down = ring(axis, here)
            oq = 1 - pair
            m_pair = self.go(here, pair, {pair_axis: oq})
            m_op = self.go(here, pair, up)
            m_om = self.go(here, pair, down)
            self.cross(here, pair)
            yield
            m_pair.wait_recv()
            m_tp = self.go(here, oq, up)
            m_tm = self.go(here, oq, down)
            self.cross(here, oq)
            yield
            m_op.wait_recv()
            m_rp = self.go(hm, pair, up)
            self.cross(hm, pair)
            m_om.wait_recv()
            self.cross(hp, pair)
            yield
            m_tm.wait_recv()
            m_rm = self.go(hp, oq, down)
            self.cross(hp, oq)
            m_tp.wait_recv()
            self.cross(hm, oq)
            yield
            m_rp.wait_recv()
            self.cross(h2, pair)
            m_rm.wait_recv()
            self.cross(h2, oq)
            yield
            self.wait_cross(len(self.crossed))
            sent(*self.started)
            yield

    def gather_l(s):
        slab = ls[s]
        return Gather(lambda h, q: slab.at[(h * 2 + q) * 2 + core], "x", x, "yl", yl, True)

    def gather_u(s):
        slab = us[s]
        return Gather(lambda h, q: slab.at[h * 2 + q], "z", z, "yh", yh, False)

    def reduce_ring(key, val, q_out, q_in, tiles, axis, here, pair_axis, pair, keep, finish):
        hp, hm, h2, up, down = ring(axis, here)
        oq = 1 - pair
        started = []
        size = slice(0, 16 + 64 * tiles)

        def send(k, v, where):
            pack(q_out.at[k], v)
            copy = remote(q_out.at[k, size, :], q_in.at[k, size, :], where, (*key, k))
            started.append(copy)
            return copy

        def got(k):
            return unpack(q_in.at[k], tiles)

        m_rp = send(0, val(h2, 0), up)
        m_rm = send(1, val(h2, 1), down)
        m_ep = send(3, val(hp, 1), up)
        m_em = send(4, val(hm, 0), down)
        yield
        m_rp.wait_recv()
        m_fp = send(2, val(hp, 0) + got(0), up)
        m_rm.wait_recv()
        m_fm = send(5, val(hm, 1) + got(1), down)
        yield
        for copy in (m_ep, m_em, m_fp, m_fm):
            copy.wait_recv()
        m_y = send(6, val(here, oq) + got(2 + oq) + got(4 + oq), {pair_axis: oq})
        keep(val(here, pair) + got(2 + pair) + got(4 + pair))
        yield
        m_y.wait_recv()
        finish(got(6))
        sent(*started)
        yield

    def reduce_direct(key, val, q_out, q_in, tiles, places, finish):
        started = []
        size = slice(0, 16 + 64 * tiles)
        for k, (where, place) in enumerate(places):
            pack(q_out.at[k], val(place))
            started.append(remote(q_out.at[k, size, :], q_in.at[k, size, :], where, (*key, k)))
        yield
        total = None
        for k, copy in enumerate(started):
            copy.wait_recv()
            v = unpack(q_in.at[k], tiles)
            total = v if total is None else total + v
        finish(total)
        sent(*started)
        yield

    row_places = [({"yh": a, "z": d}, a * 4 + d) for a, d in row_peers]
    col_places = [({"yl": a, "x": d}, d * 2 + a) for a, d in col_peers]

    def keep_row(s, i, v):
        rf[s, i] = v
        hi, lo = split(v)
        at = slice(128 * i, 128 * (i + 1))
        rh[:, at] = hi
        rl[:, at] = lo
        if s > 0:
            kh[64 * (s - 1) : 64 * s, at] = hi
            kl[64 * (s - 1) : 64 * s, at] = lo

    def keep_col(s, i, v):
        cf[s, i] = v
        if s > 0:
            hi, lo = split(v)
            kh[64 * i : 64 * (i + 1), 128 * (s - 1) : 128 * s] = hi
            kl[64 * i : 64 * (i + 1), 128 * (s - 1) : 128 * s] = lo

    def rows_part(s, part):
        b = BUF[s]
        lo, hi = PARTS.get(part, (s, 2))
        over = remote(rp.at[b, 1 - core, :, lo:hi], rcl.at[b, :, lo:hi], {"core": 1 - core},
                      ("over", b, part))
        yield
        over.wait_recv()

        def val(place):
            return rp[b, core, place, lo:hi] + rcl[b, place, lo:hi]

        def keep(v):
            rf[s, lo:hi] = v

        def finish(last):
            for i in range(lo, hi):
                keep_row(s, i, -mask_col(s, i) * (rf[s, i] + last[i - lo]))
            to_out(rf.at[s, lo:hi], out.at[s, lo + 1 : hi + 1])

        if part == "T":
            keep(val(x * 2 + yl))
            yield from reduce_direct(("rT", b), val, tq_out.at[b], tq_in.at[b], hi - lo, col_places, finish)
        else:
            p = "AB".index(part)
            yield from reduce_ring(("r", b, p), lambda h, q: val(h * 2 + q), rq_out.at[b, p], rq_in.at[b, p], hi - lo,
                                   "x", x, "yl", yl, keep, finish)
        sent(over)
        yield

    def cols_part(s, part):
        b = BUF[s]
        lo, hi = PARTS.get(part, (s, 2))

        def val(place):
            return cp[b, place, lo:hi]

        def keep(v):
            cf[s, lo:hi] = v

        def finish(last):
            for i in range(lo, hi):
                keep_col(s, i, -mask_row(s, i) * (cf[s, i] + last[i - lo]))
            to_out(cf.at[s, lo:hi], out.at[lo + 1 : hi + 1, s])

        if part == "T":
            keep(val(yh * 4 + z))
            yield from reduce_direct(("cT", b), val, vq_out.at[b], vq_in.at[b], hi - lo, row_places, finish)
        else:
            p = "AB".index(part)
            yield from reduce_ring(("c", b, p), lambda h, q: val(q * 4 + h), cq_out.at[b, p], cq_in.at[b, p], hi - lo,
                                   "z", z, "yh", yh, keep, finish)

    def diag_terms(s, part):
        b = BUF[s]
        lo, hi = PARTS.get(part, (s, 2))

        @pl.loop(0, 4)
        def _(t):
            w = ls[s][pl.ds(4 * t, 4), :, 128 * (lo - s) : 128 * (hi - s)].reshape(256, 128 * (hi - lo))
            at = slice(128 * lo, 128 * hi)
            acc = nt2(rh[:, at], rl[:, at], w)
            for q in range(2):
                if part == "A":
                    dp[b, 2 * t + q] = acc[:, 128 * q : 128 * (q + 1)]
                else:
                    dp[b, 2 * t + q] += acc[:, 128 * q : 128 * (q + 1)]

    def reduce_diag(s):
        b = BUF[s]

        def finish(total):
            v = diag[s] - dp[b, yh * 4 + z] - total[0]
            df[s] = v
            if s > 0:
                at, cols = slice(64 * (s - 1), 64 * s), slice(128 * (s - 1), 128 * s)
                for k, dk, part in zip((kh, kl), (dkh, dkl), split(v)):
                    k[at, cols] = part
                    dk[...] = jnp.zeros((128, 128), BF16)
                    dk[at, :] = part
            to_out(df.at[s], out.at[s, s])

        yield from reduce_direct(("d", b), lambda place: dp[b, place], dq_out.at[b], dq_in.at[b], 1, row_places, finish)

    def r_block(s, t, lo, hi, add, mul):
        b = BUF[s]
        acc = mul(us[s][pl.ds(2 * t, 2), :, :].reshape(256, 640 - U0[s]))
        for q in range(4):
            for i in range(lo, hi):
                v = acc[64 * q : 64 * (q + 1), 128 * (i - lo) : 128 * (i - lo + 1)]
                if add:
                    rp[b, q % 2, t + 4 * (q // 2), i] += v
                else:
                    rp[b, q % 2, t + 4 * (q // 2), i] = v

    def c_block(s, t, lo, hi, add, mul):
        b = BUF[s]
        acc = mul(ls[s][pl.ds(4 * t, 4), :, :].reshape(256, KC[s]))
        for q in range(2):
            for i in range(lo, hi):
                v = acc[64 * (i - lo) : 64 * (i - lo + 1), 128 * q : 128 * (q + 1)]
                if add:
                    cp[b, 2 * t + q, i] += v
                else:
                    cp[b, 2 * t + q, i] = v

    def heavy_c(s, t):
        def mul(w):
            w = w[:, 256 - 128 * s :]
            return nt2(kh[128:640, 256:1280], kl[128:640, 256:1280], w)

        c_block(s, t, 2, 10, False, mul)

    def heavy_r(s, t):
        def mul(w):
            w = w[:, 128 - U0[s] :]
            return nn(w, kh[128:640, 256:1280]) + nn(w, kl[128:640, 256:1280])

        r_block(s, t, 2, 10, False, mul)

    def extra_r(s, part):
        lo, hi = PARTS[part]
        at = slice(128 * lo, 128 * hi)

        @pl.loop(0, 4)
        def _(t):
            r_block(s, t, lo, hi, True, lambda w: nn2(w[:, 0:128], kh[0:128, at], kl[0:128, at]))

    def extra_c(s, part):
        lo, hi = PARTS[part]
        at, mid = slice(64 * lo, 64 * hi), slice(128 * s, 256)

        @pl.loop(0, 4)
        def _(t):
            c_block(s, t, lo, hi, True, lambda w: nt2(kh[at, mid], kl[at, mid], w[:, 0 : 256 - 128 * s]))


    def tail_r(s):
        at = slice(128 * s, 256)

        @pl.loop(0, 4)
        def _(t):
            r_block(s, t, s, 2, False, lambda w: nn2(w, kh[0:640, at], kl[0:640, at]))

    def tail_c(s):
        at, cols = slice(64 * s, 128), slice(128 * s, 1280)

        @pl.loop(0, 4)
        def _(t):
            c_block(s, t, s, 2, False, lambda w: nt2(kh[at, cols], kl[at, cols], w))

    def tail_diag(s):
        @pl.loop(0, 4)
        def _(t):
            at = slice(64 * s, 64 * (s + 1))
            r_block(s, t, s, s + 1, True, lambda w: nn2(w[:, 0:128], dkh[...], dkl[...]))
            c_block(s, t, s, s + 1, True, lambda w: nt2(dkh[at, :], dkl[at, :], w[:, 0:128]))

    gl = {s: gather_l(s) for s in (2, 1, 0)}
    gu = {s: gather_u(s) for s in (2, 1, 0)}

    def run(name, f, *args):
        with jax.named_scope(name):
            f(*args)

    def split_region():
        for b in range(8):
            loads[b].wait()
            to_out(a32.at[b], out.at[3:11, 3 + b])
            hi, lo = split(a32[b].reshape(512, 128))
            kh[128:640, (b + 2) * 128 : (b + 3) * 128] = hi
            kl[128:640, (b + 2) * 128 : (b + 3) * 128] = lo
        for ref in (kh, kl):
            ref[0:128, :] = jnp.zeros((128, 1280), BF16)
            ref[128:640, 0:256] = jnp.zeros((512, 256), BF16)

    places = {}
    for f, axis, here in ((heavy_r, "z", z), (heavy_c, "x", x)):
        up, down, far, *_ = ring(axis, here)
        places[f] = (here, up, down, far)

    def heavy(f, s, piece):
        if s == 2:
            f(s, places[f][piece])
        else:
            pl.loop(2 * piece, 2 * piece + 2)(lambda t: f(s, t))

    R = {(s, p): rows_part(s, p) for s in (2, 1, 0) for p in "ABT"}
    C = {(s, p): cols_part(s, p) for s in (2, 1, 0) for p in "ABT"}
    D = {s: reduce_diag(s) for s in (2, 1, 0)}
    actions = {
        "gl": lambda s, p: next(gl[s].steps),
        "gu": lambda s, p: next(gu[s].steps),
        "k": lambda s, p: gl[s].wait_cross(2),
        "S": lambda s, p: split_region(),
        "H": lambda s, p: heavy(heavy_r, s, int(p)),
        "h": lambda s, p: heavy(heavy_c, s, int(p)),
        "r": lambda s, p: next(R[s, p]),
        "c": lambda s, p: next(C[s, p]),
        "d": lambda s, p: next(D[s]),
        "X": extra_r,
        "x": extra_c,
        "m": diag_terms,
        "T": lambda s, p: tail_r(s),
        "t": lambda s, p: tail_c(s),
        "u": lambda s, p: tail_diag(s),
    }
    for name in " ".join(PLAN).split():
        kind = name[:2] if name[0] == "g" else name[0]
        rest = name[len(kind) :]
        run(name, actions[kind], int(rest[0]), rest[1:])
    with jax.named_scope("outs"):
        for copy in out_copies:
            copy.wait()


def pass_on(src, dst, held, in_sem, out_sem):
    into = [pltpu.make_async_copy(src.at[a], held.at[a], in_sem.at[a]) for a in range(NSEG)]
    onward = [pltpu.make_async_copy(held.at[a], dst.at[a], out_sem.at[a]) for a in range(NSEG)]
    for copy in into:
        copy.start()
    for first, second in zip(into, onward):
        first.wait()
        second.start()
    for copy in onward:
        copy.wait()


def per_device(region, l_panels, u_panels, diag_inv, pattern):
    lin = l_panels.transpose(0, 2, 1, 3)
    blocks = pattern.transpose(0, 2, 1)
    hbm = pl.BlockSpec(memory_space=pl.ANY)
    sem = lambda n: pltpu.SemaphoreType.DMA((n,))
    blocks_out = pl.pallas_call(
        kernel,
        name="selinv",
        out_shape=jax.ShapeDtypeStruct((NSEG, NSEG, 64, 128), F32),
        in_specs=[hbm] * 5,
        out_specs=hbm,
        scratch_shapes=[
            pltpu.SMEM((3, 8, NSEG), jnp.int32),
            pltpu.VMEM((3, NSEG, 64, 128), BF16),
            pltpu.VMEM((3, NSEG, 64, 128), BF16),
            pltpu.VMEM((3, 64, 128), F32),
            pltpu.VMEM((8, 8, 64, 128), F32),
            pltpu.VMEM((640, 1280), BF16),
            pltpu.VMEM((640, 1280), BF16),
            pltpu.VMEM((16, 64, KC[2]), BF16),
            pltpu.VMEM((16, 64, KC[1]), BF16),
            pltpu.VMEM((16, 64, KC[0]), BF16),
            pltpu.VMEM((8, 128, 512), BF16),
            pltpu.VMEM((8, 128, 640), BF16),
            pltpu.VMEM((8, 128, 640), BF16),
            pltpu.VMEM((2, 8, 10, 64, 128), F32),
            pltpu.VMEM((2, 2, 8, 10, 64, 128), F32),
            pltpu.VMEM((2, 8, 10, 64, 128), F32),
            pltpu.VMEM((2, 2, 7, 272, 128), I16),
            pltpu.VMEM((2, 2, 7, 272, 128), I16),
            pltpu.VMEM((2, 2, 7, 272, 128), I16),
            pltpu.VMEM((2, 2, 7, 272, 128), I16),
            pltpu.VMEM((2, 7, 80, 128), I16),
            pltpu.VMEM((2, 7, 80, 128), I16),
            pltpu.VMEM((2, 7, 144, 128), I16),
            pltpu.VMEM((2, 7, 144, 128), I16),
            pltpu.VMEM((2, 7, 144, 128), I16),
            pltpu.VMEM((2, 7, 144, 128), I16),
            pltpu.VMEM((2, 8, 64, 128), F32),
            pltpu.VMEM((3, 10, 64, 128), F32),
            pltpu.VMEM((3, 10, 64, 128), F32),
            pltpu.VMEM((3, 64, 128), F32),
            pltpu.VMEM((64, 1280), BF16),
            pltpu.VMEM((64, 1280), BF16),
            pltpu.VMEM((128, 128), BF16),
            pltpu.VMEM((128, 128), BF16),
            sem(SENDS),
            sem(RECVS),
            sem(OUTS),
        ],
        compiler_params=pltpu.CompilerParams(
            collective_id=0, has_side_effects=True, vmem_limit_bytes=64000 * 1024),
    )(blocks, region, lin, u_panels, diag_inv)
    result = pl.pallas_call(
        pass_on,
        name="pass_on",
        out_shape=jax.ShapeDtypeStruct((NSEG, NSEG, 64, 128), F32),
        in_specs=[hbm],
        out_specs=hbm,
        scratch_shapes=[pltpu.VMEM((NSEG, NSEG, 64, 128), F32), sem(NSEG), sem(NSEG)],
        compiler_params=pltpu.CompilerParams(vmem_limit_bytes=64000 * 1024),
    )(blocks_out)
    return result.transpose(0, 2, 1, 3)


def solution(mesh):
    split_mesh = Mesh(mesh.devices.reshape(2, 4, 4, 2, 2), ROW + COL)
    in_specs = (
        P(None, COL, None, ROW),
        P(None, COL, None, ROW),
        P(None, None, COL, ROW),
        P(None, COL, ROW),
        P(),
    )
    out_specs = P(None, COL, None, ROW)
    return jax.shard_map(
        per_device, mesh=split_mesh, in_specs=in_specs, out_specs=out_specs, check_vma=False
    )
```
